256 devices in a mesh: seq: 64 (over y, z, core), tensor: 4 (over x).
Axes of the slice: x: 4, y: 4, z: 8, core: 2. Of those that a mesh axis runs over, the one named last changes fastest.
Arguments:
- hidden_in: bfloat16 [8192, 8192], P('seq', 'tensor'), may hold values from -6 to 6
- grad_out: bfloat16 [8192, 8192], P('seq', 'tensor'), may hold values from -6 to 6
- slot_tokens: int32 [1024], P('seq'), may hold values from 0 to 127, as said below
- live_counts: int32 [64], P('seq'), may hold values from 5 to 16, as said below
- norm_gain: float32 [8192], P('tensor'), may hold values from 0.5 to 1.5
- router_weight: float32 [8192], P('tensor'), may hold values from -0.0625 to 0.0625
- gate_weight: bfloat16 [8192, 24576], P('tensor', 'seq'), may hold values from -0.0625 to 0.0625
- up_weight: bfloat16 [8192, 24576], P('tensor', 'seq'), may hold values from -0.0625 to 0.0625
- down_weight: bfloat16 [24576, 8192], P('seq', 'tensor'), may hold values from -0.0390625 to 0.0390625
Outputs:
- grad_in: bfloat16 [8192, 8192], P('seq', 'tensor')
- grad_gate: bfloat16 [8192, 24576], P('tensor', 'seq')
- grad_up: bfloat16 [8192, 24576], P('tensor', 'seq')
- grad_down: bfloat16 [24576, 8192], P('seq', 'tensor')
- grad_gain: float32 [8192], P('tensor')
- grad_router: float32 [8192], P('tensor')
The draws below stay inside these ranges and needn't reach their ends.
Inputs may be any that keep to these rules, and one draw needn't show every extreme that they name: `slot_tokens`: slot p belongs to index p // 16 of seq; the live slots of one index hold distinct positions, the others hold arbitrary positions of that index. `live_counts`: in every draw some index of seq has all 16 slots live.
All inputs are finite; a program needn't handle non-finite values.
Results may differ from the reference program's by a relative error of at most 0.0077.
Values may be sent and summed in bfloat16 or wider, within the bound.
A program may use at most 128 MiB of HBM per device.

```python
import jax
import jax.numpy as jnp
from jax import lax

D = 8192
FF = 24576
TOK_DEV = 128
CAP = 16
TOKENS = 8192
N_SEQ = 64


def routing_draw(key):
    base = jax.random.fold_in(key, 11)
    first, second, third, fourth = jax.random.split(base, 4)
    lowest = max(CAP // 3, 1)
    ranks = jnp.arange(N_SEQ, dtype=jnp.int32)
    floors = lowest + (CAP - lowest) * ranks // max(N_SEQ - 1, 1)
    counts = jax.random.randint(first, (N_SEQ,), floors, CAP + 1, dtype=jnp.int32)
    chosen = jax.random.randint(second, (), 0, N_SEQ, dtype=jnp.int32)
    counts = jnp.where(ranks == chosen, CAP, counts).astype(jnp.int32)
    keys = jax.random.split(third, N_SEQ)
    orders = jax.vmap(lambda single: jax.random.permutation(single, TOK_DEV))(keys)[:, :CAP].astype(jnp.int32)
    filler = jax.random.randint(fourth, (N_SEQ, CAP), 0, TOK_DEV, dtype=jnp.int32)
    columns = jnp.arange(CAP, dtype=jnp.int32)[None, :]
    tokens = jnp.where(columns < counts[:, None], orders, filler).reshape(-1).astype(jnp.int32)
    return (tokens, counts)


def draw_slot_tokens(key, part):
    return routing_draw(key)[0]


def draw_live_counts(key, part):
    return routing_draw(key)[1]


def block_scale(own_key, shape, pieces, least, top_value):
    def one(dim, blocks):
        heights = jax.random.uniform(jax.random.fold_in(jax.random.fold_in(own_key, 6), dim), (blocks,), jnp.float32, least / len(pieces), top_value / len(pieces))
        return jnp.repeat(jnp.exp(heights), shape[dim] // blocks).reshape((-1,) + (1,) * (len(shape) - dim - 1))

    loudness = one(*pieces[0])
    for cut in pieces[1:]:
        loudness = loudness * one(*cut)
    return loudness


def centred(stream_key, extent, spread, bound, cuts=(), kind=jnp.bfloat16):
    array = jax.random.normal(stream_key, extent, jnp.float32) * spread
    if len(cuts) > 0:
        array = block_scale(stream_key, extent, cuts, -0.22, 0.18) * array
    return jnp.clip(array, min=-bound, max=bound).astype(kind)


def setup_inputs(seed: int = 0) -> dict:
    key_list = jax.random.split(jax.random.key(seed), 10)
    return {
        "hidden_in": centred(key_list[0], (TOKENS, D), 1.0, 6.0, ((0, 64), (1, 4))),
        "grad_out": centred(key_list[1], (TOKENS, D), 1.0, 6.0, ((0, 64), (1, 4))),
        "slot_tokens": draw_slot_tokens(jax.random.fold_in(key_list[9], 71), 0),
        "live_counts": draw_live_counts(jax.random.fold_in(key_list[9], 71), 0),
        "norm_gain": jnp.clip(1.0 + 0.1 * jax.random.normal(key_list[4], (D,), jnp.float32), 0.5, 1.5),
        "router_weight": centred(key_list[5], (D,), D ** -0.5, 0.0625, ((0, 4),), jnp.float32),
        "gate_weight": centred(key_list[6], (D, FF), D ** -0.5, 0.0625, ((0, 4), (1, 64))),
        "up_weight": centred(key_list[7], (D, FF), D ** -0.5, 0.0625, ((0, 4), (1, 64))),
        "down_weight": centred(key_list[8], (FF, D), FF ** -0.5, 0.0390625, ((0, 64), (1, 4))),
    }


norm_eps = 1e-06

def silu_parts(gate):
    sig = jax.nn.sigmoid(gate)
    return (gate * sig, sig * (1.0 + gate * (1.0 - sig)))

def reference(hidden_in, grad_out, slot_tokens, live_counts, norm_gain, router_weight, gate_weight, up_weight, down_weight):
    slots = jnp.arange(N_SEQ * CAP, dtype=jnp.int32)
    owners = slots // CAP
    positions = (owners * TOK_DEV + slot_tokens).astype(jnp.int32)
    live_rows = slots % CAP < live_counts[owners]
    picked = jnp.take(hidden_in, positions, axis=0)
    upstream = jnp.where(live_rows[:, None], jnp.take(grad_out, positions, axis=0), jnp.zeros((), jnp.bfloat16))
    wide = picked.astype(jnp.float32)
    inverse = lax.rsqrt(lax.optimization_barrier(jnp.mean(wide * wide, axis=1, keepdims=True)) + norm_eps)
    scaled = wide * inverse
    normed = (scaled * norm_gain).astype(jnp.bfloat16)
    logits = jnp.dot(normed, router_weight.astype(jnp.bfloat16), preferred_element_type=jnp.float32)
    gate = jnp.dot(normed, gate_weight, preferred_element_type=jnp.float32)
    upper = jnp.dot(normed, up_weight, preferred_element_type=jnp.float32)
    back = jnp.dot(upstream, down_weight.T, preferred_element_type=jnp.float32)
    act, slope = silu_parts(gate)
    hidden = act * upper
    weighted = (hidden * logits[:, None]).astype(jnp.bfloat16)
    router_grad = lax.optimization_barrier(jnp.sum(hidden * back, axis=1))
    d_hidden = logits[:, None] * back
    d_gate = (d_hidden * upper * slope).astype(jnp.bfloat16)
    d_up = (d_hidden * act).astype(jnp.bfloat16)
    count_scale = lax.rsqrt(jnp.sum(live_counts).astype(jnp.float32))
    grad_gate = (count_scale * jnp.dot(normed.T, d_gate, preferred_element_type=jnp.float32)).astype(jnp.bfloat16)
    grad_up = (count_scale * jnp.dot(normed.T, d_up, preferred_element_type=jnp.float32)).astype(jnp.bfloat16)
    grad_down = (count_scale * jnp.dot(weighted.T, upstream, preferred_element_type=jnp.float32)).astype(jnp.bfloat16)
    d_normed = jnp.dot(d_gate, gate_weight.T, preferred_element_type=jnp.float32)
    d_normed = d_normed + jnp.dot(d_up, up_weight.T, preferred_element_type=jnp.float32)
    d_normed = d_normed + router_grad[:, None] * router_weight
    grad_gain = count_scale * lax.optimization_barrier(jnp.sum(d_normed * scaled, axis=0))
    grad_router = count_scale * jnp.dot(router_grad, normed.astype(jnp.float32), precision=lax.Precision.HIGHEST)
    d_scaled = d_normed * norm_gain
    d_picked = inverse * (d_scaled - scaled * lax.optimization_barrier(jnp.mean(d_scaled * scaled, axis=1, keepdims=True)))
    d_picked = jnp.where(live_rows[:, None], d_picked, jnp.zeros((), jnp.float32))
    grad_in = grad_out.astype(jnp.float32).at[positions].add(d_picked).astype(jnp.bfloat16)
    return (grad_in, grad_gate, grad_up, grad_down, grad_gain, grad_router)
```

```python
import functools

import jax
import jax.numpy as jnp
from jax import lax
from jax.experimental import pallas as pl
from jax.experimental.pallas import tpu as pltpu
from jax.sharding import PartitionSpec as P

MESH = pl.DeviceIdType.MESH
BF = jnp.bfloat16
F32 = jnp.float32
norm_eps = 1e-06
NC = 2
CAP = 16
AUX = 128
TOK = 128


def geometry(ny, nz, nx):
    s, t = lax.axis_index("seq"), lax.axis_index("tensor")
    c = lax.rem(s, NC)
    z = lax.rem(s // NC, nz)
    y = s // (NC * nz)
    way = 1 - 2 * c
    return y, z, c, t, way


def around(value, size):
    return lax.rem(value + 8 * size, size)


def step_of(k, way):
    far = (k + 1) // 2
    sign = (2 * lax.rem(k, 2) - 1) * way
    return sign, sign * far


def pair(value):
    high = value.astype(BF)
    return high, (value - high.astype(F32)).astype(BF)


def lanes(rows, columns):
    lane = lax.broadcasted_iota(jnp.int32, (rows, AUX), 1)
    total = jnp.zeros((rows, AUX), F32)
    for k, column in enumerate(columns):
        total = jnp.where(lane == k, jnp.broadcast_to(column, (rows, AUX)), total)
    return total


def dot(a, b, contract):
    return lax.dot_general(a, b, ((contract[0:1], contract[1:2]), ((), ())), preferred_element_type=F32)


def forward_kernel(
    sizes,
    tok, cnt, hid, gro, gain, rw, wg, wu, wd,
    N, U, G, scaled_o, inv_o,
    sq, sb, rb_a, rb_b, rb_s,
    sem_sq, sem_nz, sem_ny, sem_uz, sem_uy, sem_dn, sem_du,
    sem_a, sem_b, sem_s, sem_g1, sem_g2, sem_gs, sent,
):
    ny, nz, nx, width = sizes
    y, z, c, t, way = geometry(ny, nz, nx)
    wd_cols = hid.shape[1]
    ff = wg.shape[1]
    rows = NC * CAP

    def dev(yy, zz, cc, tt):
        return ((yy * nz + zz) * NC + cc, tt)

    def copy(src, dst, send, recv, to):
        return pltpu.make_async_remote_copy(
            src_ref=src, dst_ref=dst, send_sem=sent.at[send], recv_sem=recv, device_id=to, device_id_type=MESH
        )

    partner = dev(y, z, 1 - c, t)
    y_to = lambda d: dev(around(y + d, ny), z, c, t)
    z_to = lambda d: dev(y, around(z + d, nz), c, t)
    x_to = lambda d: dev(y, z, c, around(t + d, nx))

    barrier = pltpu.get_barrier_semaphore()
    for to in (y_to(1), y_to(-1), z_to(1), z_to(-1), partner, x_to(1), x_to(2), x_to(3)):
        pl.semaphore_signal(barrier, inc=1, device_id=to, device_id_type=MESH)

    hot = (tok[...] == lax.broadcasted_iota(jnp.int32, tok.shape, 1)).astype(F32).astype(BF)
    wide = dot(hot, hid[...], (1, 0))
    ups = dot(hot, gro[...], (1, 0))
    live = lax.broadcasted_iota(jnp.int32, (CAP, AUX), 0) < cnt[...]
    rounded = rw[...].astype(BF).astype(F32)
    s1 = jnp.sum(wide * wide, axis=1, keepdims=True)
    s2 = jnp.sum(wide * (gain[...] * rounded), axis=1, keepdims=True)
    sq[t] = lanes(CAP, (s1, s2))

    pl.semaphore_wait(barrier, 8)
    for d in (1, 2, 3):
        copy(sq.at[t], sq.at[t], 0, sem_sq.at[t], x_to(d)).start()
    U[z, y, c, :, 0:wd_cols] = jnp.where(live[:, 0:1], ups, 0.0).astype(BF)
    for d in (1, 2, 3):
        frm = around(t + d, nx)
        copy(sq.at[frm], sq.at[frm], 0, sem_sq.at[frm], x_to(1)).wait_recv()
    total = sq[0]
    for k in range(1, nx):
        total = total + sq[k]
    inverse = lax.rsqrt(total[:, 0:1] / width + norm_eps)
    scaled = wide * inverse
    N[z, y, c] = (scaled * gain[...]).astype(BF)
    scaled_o[...] = scaled
    inv_o[...] = jnp.broadcast_to(inverse, (CAP, AUX))
    high, low = pair(total[:, 1:2] * inverse)
    U[z, y, c, :, wd_cols:] = lanes(CAP, (high.astype(F32), low.astype(F32), cnt[:, 0:1].astype(F32))).astype(BF)

    def n_copy(zz, yy, send, recv, to):
        block = N.at[zz, yy, c]
        return copy(block, block, send, recv, to)

    def u_copy(zz, yy, send, recv, to):
        block = U.at[zz, yy, c]
        return copy(block, block, send, recv, to)

    def n_z_sends(yy):
        n_copy(z, yy, 2, sem_nz.at[1, yy], z_to(way)).start()
        if nz > 2:
            n_copy(z, yy, 2, sem_nz.at[2, yy], z_to(-way)).start()

    def u_y_sends(zz):
        u_copy(zz, y, 4, sem_uy.at[1, zz], y_to(way)).start()
        if ny > 2:
            u_copy(zz, y, 4, sem_uy.at[2, zz], y_to(-way)).start()

    n_copy(z, y, 1, sem_ny.at[1], y_to(way)).start()
    if ny > 2:
        n_copy(z, y, 1, sem_ny.at[2], y_to(-way)).start()
    u_copy(z, y, 3, sem_uz.at[1], z_to(way)).start()
    if nz > 2:
        u_copy(z, y, 3, sem_uz.at[2], z_to(-way)).start()
    n_z_sends(y)
    u_y_sends(z)

    for m in range(1, ny):
        sign, far = step_of(m, way)
        yy = around(y - far, ny)
        n_copy(z, yy, 1, sem_ny.at[m], y_to(sign)).wait_recv()
        if m + 2 < ny:
            n_copy(z, yy, 1, sem_ny.at[m + 2], y_to(sign)).start()
        n_z_sends(yy)
    copy(N.at[z, :, c], N.at[z, :, c], 5, sem_dn.at[z], partner).start()

    def chunk_z(k):
        return around(z - step_of(k, way)[1], nz)

    def u_y_arrival(k, m):
        zz = chunk_z(k)
        sign, far = step_of(m, way)
        yy = around(y - far, ny)
        u_copy(zz, yy, 4, sem_uy.at[m, zz], y_to(sign)).wait_recv()
        if m + 2 < ny:
            u_copy(zz, yy, 4, sem_uy.at[m + 2, zz], y_to(sign)).start()

    def x_block(i, d):
        return sb.at[i, around(t + d, nx)]

    def loop(k, carry):
        @pl.when((k >= 1) & (k < nz))
        def _():
            sign, far = step_of(k, way)
            zz = around(z - far, nz)
            to = z_to(sign)
            u_copy(zz, y, 3, sem_uz.at[k], to).wait_recv()

            @pl.when(k + 2 < nz)
            def _():
                u_copy(zz, y, 3, sem_uz.at[k + 2], to).start()

            u_y_sends(zz)
            for yy in range(ny):
                n_copy(zz, yy, 2, sem_nz.at[k, yy], to).wait_recv()

                @pl.when(k + 2 < nz)
                def _():
                    n_copy(zz, yy, 2, sem_nz.at[k + 2, yy], to).start()

            copy(N.at[zz, :, c], N.at[zz, :, c], 5, sem_dn.at[zz], partner).start()

        @pl.when((k >= 1) & (k - 1 < nz))
        def _():
            for m in range(1, min(ny, 3)):
                u_y_arrival(k - 1, m)

        @pl.when((k >= 2) & (k - 2 < nz))
        def _():
            for m in range(3, ny):
                u_y_arrival(k - 2, m)
            zz = chunk_z(k - 2)
            copy(U.at[zz, :, c], U.at[zz, :, c], 6, sem_du.at[zz], partner).start()

        @pl.when((k >= 4) & (k - 4 < nz))
        def _():
            i = k - 4
            block = x_block(i, way)
            copy(block, rb_a.at[i], 7, sem_a.at[i], x_to(way)).wait_recv()
            ref = sb.at[i, around(t + way, nx)]
            ref[...] = (ref[...].astype(F32) + rb_a[i].astype(F32)).astype(BF)
            copy(block, rb_b.at[i], 7, sem_b.at[i], x_to(way)).start()

        @pl.when((k >= 3) & (k - 3 < nz))
        def _():
            i = k - 3
            zz = chunk_z(i)
            other_n = N.at[zz, :, 1 - c]
            other_u = U.at[zz, :, 1 - c]
            copy(other_n, other_n, 5, sem_dn.at[zz], partner).wait_recv()
            copy(other_u, other_u, 6, sem_du.at[zz], partner).wait_recv()
            n = N[zz].reshape(ny * rows, wd_cols)
            u = U[zz, :, :, :, 0:wd_cols].reshape(ny * rows, wd_cols)
            for q, part in enumerate((dot(n, wg[...], (1, 0)), dot(n, wu[...], (1, 0)), dot(u, wd[...], (1, 1)))):
                sb[i, :, :, q * ff:(q + 1) * ff] = part.astype(BF).reshape(nx, rows, ff)
            copy(x_block(i, 2), rb_a.at[i], 7, sem_a.at[i], x_to(way)).start()
            copy(x_block(i, -way), rb_s.at[i], 7, sem_s.at[i], x_to(-way)).start()

        @pl.when((k >= 6) & (k - 6 < nz))
        def _():
            i = k - 6
            zz = chunk_z(i)
            block = G.at[zz, around(t - way, nx)]
            copy(block, block, 8, sem_g1.at[i], x_to(way)).wait_recv()
            copy(block, block, 8, sem_g2.at[i], x_to(way)).start()

        @pl.when((k >= 5) & (k - 5 < nz))
        def _():
            i = k - 5
            zz = chunk_z(i)
            block = x_block(i, 0)
            copy(block, rb_b.at[i], 7, sem_b.at[i], x_to(way)).wait_recv()
            copy(block, rb_s.at[i], 7, sem_s.at[i], x_to(-way)).wait_recv()
            full = sb[i, t].astype(F32) + rb_b[i].astype(F32) + rb_s[i].astype(F32)
            gate, upper, back = full[:, 0:ff], full[:, ff:2 * ff], full[:, 2 * ff:]
            aux = U[zz, t, :, :, wd_cols:].reshape(rows, AUX).astype(F32)
            logits = aux[:, 0:1] + aux[:, 1:2]
            sig = jax.nn.sigmoid(gate)
            act = gate * sig
            slope = sig * (1.0 + gate * (1.0 - sig))
            hidden = act * upper
            d_hidden = logits * back
            d_gate = (d_hidden * upper * slope).astype(BF)
            d_up = (d_hidden * act).astype(BF)
            router = jnp.sum(hidden * back, axis=1, keepdims=True)
            inner = jnp.sum(d_gate.astype(F32) * gate + d_up.astype(F32) * upper, axis=1, keepdims=True) + router * logits
            G[zz, t, :, 0:ff] = d_gate
            G[zz, t, :, ff:2 * ff] = d_up
            G[zz, t, :, 2 * ff:3 * ff] = (hidden * logits).astype(BF)
            rh, rl = pair(router)
            ih, il = pair(inner)
            G[zz, t, :, 3 * ff:] = lanes(rows, [v.astype(F32) for v in (rh, rl, ih, il)]).astype(BF)
            mine = G.at[zz, t]
            copy(mine, mine, 8, sem_g1.at[i], x_to(way)).start()
            copy(mine, mine, 8, sem_gs.at[i], x_to(-way)).start()

        @pl.when((k >= 7) & (k - 7 < nz))
        def _():
            i = k - 7
            zz = chunk_z(i)
            block = G.at[zz, around(t + way, nx)]
            copy(block, block, 8, sem_gs.at[i], x_to(way)).wait_recv()
            block = G.at[zz, around(t + 2, nx)]
            copy(block, block, 8, sem_g2.at[i], x_to(way)).wait_recv()

        return carry

    lax.fori_loop(0, nz + 7, loop, 0)

    def drain(ref, send):
        copy(ref, ref, send, sem_sq.at[0], partner).wait_send()

    drain(sq.at[0:3], 0)
    drain(N.at[0, 0:ny - 1, 0], 1)
    drain(N.at[0:nz - 1, :, 0], 2)
    drain(U.at[0:nz - 1, 0, 0], 3)
    drain(U.at[:, 0:ny - 1, 0], 4)
    drain(N.at[:, :, 0], 5)
    drain(U.at[:, :, 0], 6)
    drain(sb.at[:, 0:3], 7)
    drain(G.at[:, 0:3], 8)


def forward(sizes, tok, cnt, hid, gro, gain, rw, wg, wu, wd):
    ny, nz, nx, width = sizes
    cols, ff = wg.shape
    rows = NC * CAP
    vmem = pl.BlockSpec(memory_space=pltpu.VMEM)
    dma = pltpu.SemaphoreType.DMA
    return pl.pallas_call(
        functools.partial(forward_kernel, sizes),
        out_shape=(
            jax.ShapeDtypeStruct((nz, ny, NC, CAP, cols), BF),
            jax.ShapeDtypeStruct((nz, ny, NC, CAP, cols + AUX), BF),
            jax.ShapeDtypeStruct((nz, nx, rows, 3 * ff + AUX), BF),
            jax.ShapeDtypeStruct((CAP, cols), F32),
            jax.ShapeDtypeStruct((CAP, AUX), F32),
        ),
        in_specs=[vmem] * 9,
        out_specs=[vmem] * 5,
        scratch_shapes=[
            pltpu.VMEM((nx, CAP, AUX), F32),
            pltpu.VMEM((nz, nx, rows, 3 * ff), BF),
            pltpu.VMEM((nz, rows, 3 * ff), BF),
            pltpu.VMEM((nz, rows, 3 * ff), BF),
            pltpu.VMEM((nz, rows, 3 * ff), BF),
            dma((nx,)), dma((nz, ny)), dma((ny,)), dma((nz,)), dma((ny, nz)), dma((nz,)), dma((nz,)),
            dma((nz,)), dma((nz,)), dma((nz,)), dma((nz,)), dma((nz,)), dma((nz,)), dma((9,)),
        ],
        compiler_params=pltpu.CompilerParams(collective_id=0, has_side_effects=True, vmem_limit_bytes=64000000),
        name="forward",
    )(tok, cnt, hid, gro, gain, rw, wg, wu, wd)


def body(hidden_in, grad_out, slot_tokens, live_counts, norm_gain, router_weight, gate_weight, up_weight, down_weight, sizes):
    ny, nz, nx, width = sizes
    ff = gate_weight.shape[1]
    cols = hidden_in.shape[1]
    tok = jnp.broadcast_to(slot_tokens[:, None], (CAP, TOK))
    cnt = jnp.broadcast_to(live_counts[:, None], (CAP, AUX))
    N, U, G, scaled, inv = forward(
        sizes, tok, cnt, hidden_in, grad_out, norm_gain[None], router_weight[None], gate_weight, up_weight, down_weight
    )
    slots = nz * ny * NC * CAP
    n = N.reshape(slots, cols)
    u = U[..., :cols].reshape(slots, cols)
    aux = G[..., 3 * ff:].astype(F32)
    g = G.reshape(slots, -1)
    d_gate, d_up, weighted = g[:, :ff], g[:, ff:2 * ff], g[:, 2 * ff:3 * ff]
    rg = (aux[..., 0] + aux[..., 1]).reshape(slots)
    count_scale = lax.rsqrt(jnp.sum(U[:, :, :, 0, cols + 2].astype(F32)))
    grad_gate = jnp.einsum("pd,pf->df", n, d_gate, preferred_element_type=F32)
    grad_up = jnp.einsum("pd,pf->df", n, d_up, preferred_element_type=F32)
    grad_down = jnp.einsum("pf,pd->fd", weighted, u, preferred_element_type=F32)
    router_part = jnp.dot(rg, n.astype(F32), precision=lax.Precision.HIGHEST)
    total = jnp.einsum("pf,df->pd", d_gate, gate_weight, preferred_element_type=F32)
    total = total + jnp.einsum("pf,df->pd", d_up, up_weight, preferred_element_type=F32)
    total = (total + rg[:, None] * router_weight).astype(BF)
    parts = jnp.moveaxis(total.reshape(nz, ny, NC, CAP, cols), 0, 1).reshape(-1, CAP, cols)
    d_normed = lax.all_to_all(parts, "seq", 0, 0, tiled=True).astype(F32).sum(axis=0)
    d_scaled = d_normed * norm_gain
    inner = lax.psum(jnp.sum(d_scaled * scaled, axis=1), "tensor") / width
    live = lax.iota(jnp.int32, CAP) < live_counts[0]
    d_picked = inv[:, 0:1] * (d_scaled - scaled * inner[:, None])
    d_picked = jnp.where(live[:, None], d_picked, 0.0)
    sums = lax.psum(jnp.concatenate([jnp.sum(d_normed * scaled, axis=0), router_part]), "seq")
    grad_in = grad_out.astype(F32).at[slot_tokens].add(d_picked).astype(BF)
    return (
        grad_in,
        (count_scale * grad_gate).astype(BF),
        (count_scale * grad_up).astype(BF),
        (count_scale * grad_down).astype(BF),
        count_scale * sums[:cols],
        count_scale * sums[cols:],
    )


def solution(mesh):
    nx = mesh.shape["tensor"]
    ny = nx
    nz = mesh.shape["seq"] // (ny * NC)
    weights = (P("tensor", "seq"), P("tensor", "seq"), P("seq", "tensor"))
    in_specs = (P("seq", "tensor"), P("seq", "tensor"), P("seq"), P("seq"), P("tensor"), P("tensor")) + weights
    out_specs = (P("seq", "tensor"),) + weights + (P("tensor"), P("tensor"))

    def whole(hidden_in, *rest):
        sizes = (ny, nz, nx, hidden_in.shape[1] * nx)
        return body(hidden_in, *rest, sizes)

    return jax.shard_map(whole, mesh=mesh, in_specs=in_specs, out_specs=out_specs, check_vma=False)
```

```python
import functools

import jax
import jax.numpy as jnp
from jax import lax
from jax.experimental import pallas as pl
from jax.experimental.pallas import tpu as pltpu
from jax.sharding import PartitionSpec as P

MESH = pl.DeviceIdType.MESH
BF = jnp.bfloat16
F32 = jnp.float32
norm_eps = 1e-06
NC = 2
CAP = 16
AUX = 128
TOK = 128
TILE = 256


def geometry(ny, nz, nx):
    s, t = lax.axis_index("seq"), lax.axis_index("tensor")
    c = lax.rem(s, NC)
    z = lax.rem(s // NC, nz)
    y = s // (NC * nz)
    way = 1 - 2 * c
    return y, z, c, t, way


def around(value, size):
    return lax.rem(value + 8 * size, size)


def step_of(k, way):
    far = (k + 1) // 2
    sign = (2 * lax.rem(k, 2) - 1) * way
    return sign, sign * far


def pair(value):
    high = value.astype(BF)
    return high, (value - high.astype(F32)).astype(BF)


def lanes(rows, columns):
    lane = lax.broadcasted_iota(jnp.int32, (rows, AUX), 1)
    total = jnp.zeros((rows, AUX), F32)
    for k, column in enumerate(columns):
        total = jnp.where(lane == k, jnp.broadcast_to(column, (rows, AUX)), total)
    return total


def dot(a, b, contract):
    return lax.dot_general(a, b, ((contract[0:1], contract[1:2]), ((), ())), preferred_element_type=F32)


def kernel(
    sizes,
    tok, tok_row, cnt, hid, gro, gain, rw, wg, wu, wd,
    grad_in, grad_gate, grad_up, grad_down, grad_gain, grad_router,
    N, U, G, scaled_o, inv_o,
    sq, sb, rb_a, rb_b, rb_s,
    t_a, t_b, acc_a, acc_b, a1l, a1s, a2l, a2s, b1l, b1s, b2l, b2s, v_acc, v_own, v_core, v_y, v_z,
    sem_sq, sem_nz, sem_ny, sem_uz, sem_uy, sem_dn, sem_du,
    sem_a, sem_b, sem_s, sem_g1, sem_g2, sem_gs,
    sem_ta, sem_tb, sem_a1, sem_a2, sem_b1, sem_b2, sem_v, sem_vy, sem_vz, sent,
):
    ny, nz, nx, width = sizes
    y, z, c, t, way = geometry(ny, nz, nx)
    wd_cols = hid.shape[1]
    ff = wg.shape[1]
    rows = NC * CAP

    def dev(yy, zz, cc, tt):
        return ((yy * nz + zz) * NC + cc, tt)

    def copy(src, dst, send, recv, to):
        return pltpu.make_async_remote_copy(
            src_ref=src, dst_ref=dst, send_sem=sent.at[send], recv_sem=recv, device_id=to, device_id_type=MESH
        )

    partner = dev(y, z, 1 - c, t)
    y_to = lambda d: dev(around(y + d, ny), z, c, t)
    z_to = lambda d: dev(y, around(z + d, nz), c, t)
    x_to = lambda d: dev(y, z, c, around(t + d, nx))

    barrier = pltpu.get_barrier_semaphore()
    peers = [y_to(d) for d in range(1, ny)] + [z_to(d) for d in range(1, nz)] + [x_to(d) for d in range(1, nx)] + [partner]
    for to in peers:
        pl.semaphore_signal(barrier, inc=1, device_id=to, device_id_type=MESH)

    hot = (tok[...] == lax.broadcasted_iota(jnp.int32, tok.shape, 1)).astype(F32).astype(BF)
    wide = dot(hot, hid[...], (1, 0))
    ups = dot(hot, gro[...], (1, 0))
    live = lax.broadcasted_iota(jnp.int32, (CAP, AUX), 0) < cnt[...]
    rounded = rw[...].astype(BF).astype(F32)
    s1 = jnp.sum(wide * wide, axis=1, keepdims=True)
    s2 = jnp.sum(wide * (gain[...] * rounded), axis=1, keepdims=True)
    sq[t] = lanes(CAP, (s1, s2))

    pl.semaphore_wait(barrier, len(peers))
    for d in (1, 2, 3):
        copy(sq.at[t], sq.at[t], 0, sem_sq.at[t], x_to(d)).start()
    U[z, y, c, :, 0:wd_cols] = jnp.where(live[:, 0:1], ups, 0.0).astype(BF)
    for d in (1, 2, 3):
        frm = around(t + d, nx)
        copy(sq.at[frm], sq.at[frm], 0, sem_sq.at[frm], x_to(1)).wait_recv()
    total = sq[0]
    for k in range(1, nx):
        total = total + sq[k]
    inverse = lax.rsqrt(total[:, 0:1] / width + norm_eps)
    scaled = wide * inverse
    N[z, y, c] = (scaled * gain[...]).astype(BF)
    scaled_o[...] = scaled
    inv_o[...] = jnp.broadcast_to(inverse, (CAP, AUX))
    high, low = pair(total[:, 1:2] * inverse)
    U[z, y, c, :, wd_cols:] = lanes(CAP, (high.astype(F32), low.astype(F32), cnt[:, 0:1].astype(F32))).astype(BF)

    def n_copy(zz, yy, send, recv, to):
        block = N.at[zz, yy, c]
        return copy(block, block, send, recv, to)

    def u_copy(zz, yy, send, recv, to):
        block = U.at[zz, yy, c]
        return copy(block, block, send, recv, to)

    def n_z_sends(yy):
        n_copy(z, yy, 2, sem_nz.at[1, yy], z_to(way)).start()
        if nz > 2:
            n_copy(z, yy, 2, sem_nz.at[2, yy], z_to(-way)).start()

    def u_y_sends(zz):
        u_copy(zz, y, 4, sem_uy.at[1, zz], y_to(way)).start()
        if ny > 2:
            u_copy(zz, y, 4, sem_uy.at[2, zz], y_to(-way)).start()

    n_copy(z, y, 1, sem_ny.at[1], y_to(way)).start()
    if ny > 2:
        n_copy(z, y, 1, sem_ny.at[2], y_to(-way)).start()
    u_copy(z, y, 3, sem_uz.at[1], z_to(way)).start()
    if nz > 2:
        u_copy(z, y, 3, sem_uz.at[2], z_to(-way)).start()
    n_z_sends(y)
    u_y_sends(z)

    for m in range(1, ny):
        sign, far = step_of(m, way)
        yy = around(y - far, ny)
        n_copy(z, yy, 1, sem_ny.at[m], y_to(sign)).wait_recv()
        if m + 2 < ny:
            n_copy(z, yy, 1, sem_ny.at[m + 2], y_to(sign)).start()
        n_z_sends(yy)
    copy(N.at[z, :, c], N.at[z, :, c], 5, sem_dn.at[z], partner).start()

    def chunk_z(k):
        return around(z - step_of(k, way)[1], nz)

    def u_y_arrival(k, m):
        zz = chunk_z(k)
        sign, far = step_of(m, way)
        yy = around(y - far, ny)
        u_copy(zz, yy, 4, sem_uy.at[m, zz], y_to(sign)).wait_recv()
        if m + 2 < ny:
            u_copy(zz, yy, 4, sem_uy.at[m + 2, zz], y_to(sign)).start()

    def x_block(i, d):
        return sb.at[i, around(t + d, nx)]

    def loop(k, carry):
        @pl.when((k >= 1) & (k < nz))
        def _():
            sign, far = step_of(k, way)
            zz = around(z - far, nz)
            to = z_to(sign)
            u_copy(zz, y, 3, sem_uz.at[k], to).wait_recv()

            @pl.when(k + 2 < nz)
            def _():
                u_copy(zz, y, 3, sem_uz.at[k + 2], to).start()

            u_y_sends(zz)
            for yy in range(ny):
                n_copy(zz, yy, 2, sem_nz.at[k, yy], to).wait_recv()

                @pl.when(k + 2 < nz)
                def _():
                    n_copy(zz, yy, 2, sem_nz.at[k + 2, yy], to).start()

            copy(N.at[zz, :, c], N.at[zz, :, c], 5, sem_dn.at[zz], partner).start()

        @pl.when((k >= 1) & (k - 1 < nz))
        def _():
            for m in range(1, min(ny, 3)):
                u_y_arrival(k - 1, m)

        @pl.when((k >= 2) & (k - 2 < nz))
        def _():
            for m in range(3, ny):
                u_y_arrival(k - 2, m)
            zz = chunk_z(k - 2)
            copy(U.at[zz, :, c], U.at[zz, :, c], 6, sem_du.at[zz], partner).start()

        @pl.when((k >= 4) & (k - 4 < nz))
        def _():
            i = k - 4
            block = x_block(i, way)
            copy(block, rb_a.at[i], 7, sem_a.at[i], x_to(way)).wait_recv()
            ref = sb.at[i, around(t + way, nx)]
            ref[...] = (ref[...].astype(F32) + rb_a[i].astype(F32)).astype(BF)
            copy(block, rb_b.at[i], 7, sem_b.at[i], x_to(way)).start()

        @pl.when((k >= 3) & (k - 3 < nz))
        def _():
            i = k - 3
            zz = chunk_z(i)
            other_n = N.at[zz, :, 1 - c]
            other_u = U.at[zz, :, 1 - c]
            copy(other_n, other_n, 5, sem_dn.at[zz], partner).wait_recv()
            copy(other_u, other_u, 6, sem_du.at[zz], partner).wait_recv()
            n = N[zz].reshape(ny * rows, wd_cols)
            u = U[zz, :, :, :, 0:wd_cols].reshape(ny * rows, wd_cols)
            for q, part in enumerate((dot(n, wg[...], (1, 0)), dot(n, wu[...], (1, 0)), dot(u, wd[...], (1, 1)))):
                sb[i, :, :, q * ff:(q + 1) * ff] = part.astype(BF).reshape(nx, rows, ff)
            copy(x_block(i, 2), rb_a.at[i], 7, sem_a.at[i], x_to(way)).start()
            copy(x_block(i, -way), rb_s.at[i], 7, sem_s.at[i], x_to(-way)).start()

        @pl.when((k >= 6) & (k - 6 < nz))
        def _():
            i = k - 6
            zz = chunk_z(i)
            block = G.at[zz, around(t - way, nx)]
            copy(block, block, 8, sem_g1.at[i], x_to(way)).wait_recv()
            copy(block, block, 8, sem_g2.at[i], x_to(way)).start()

        @pl.when((k >= 5) & (k - 5 < nz))
        def _():
            i = k - 5
            zz = chunk_z(i)
            block = x_block(i, 0)
            copy(block, rb_b.at[i], 7, sem_b.at[i], x_to(way)).wait_recv()
            copy(block, rb_s.at[i], 7, sem_s.at[i], x_to(-way)).wait_recv()
            full = sb[i, t].astype(F32) + rb_b[i].astype(F32) + rb_s[i].astype(F32)
            gate, upper, back = full[:, 0:ff], full[:, ff:2 * ff], full[:, 2 * ff:]
            aux = U[zz, t, :, :, wd_cols:].reshape(rows, AUX).astype(F32)
            logits = aux[:, 0:1] + aux[:, 1:2]
            sig = jax.nn.sigmoid(gate)
            act = gate * sig
            slope = sig * (1.0 + gate * (1.0 - sig))
            hidden = act * upper
            d_hidden = logits * back
            d_gate = (d_hidden * upper * slope).astype(BF)
            d_up = (d_hidden * act).astype(BF)
            router = jnp.sum(hidden * back, axis=1, keepdims=True)
            inner = jnp.sum(d_gate.astype(F32) * gate + d_up.astype(F32) * upper, axis=1, keepdims=True) + router * logits
            G[zz, t, :, 0:ff] = d_gate
            G[zz, t, :, ff:2 * ff] = d_up
            G[zz, t, :, 2 * ff:3 * ff] = (hidden * logits).astype(BF)
            rh, rl = pair(router)
            ih, il = pair(inner)
            G[zz, t, :, 3 * ff:] = lanes(rows, [v.astype(F32) for v in (rh, rl, ih, il)]).astype(BF)
            mine = G.at[zz, t]
            copy(mine, mine, 8, sem_g1.at[i], x_to(way)).start()
            copy(mine, mine, 8, sem_gs.at[i], x_to(-way)).start()

        @pl.when((k >= 7) & (k - 7 < nz))
        def _():
            i = k - 7
            zz = chunk_z(i)
            block = G.at[zz, around(t + way, nx)]
            copy(block, block, 8, sem_gs.at[i], x_to(way)).wait_recv()
            block = G.at[zz, around(t + 2, nx)]
            copy(block, block, 8, sem_g2.at[i], x_to(way)).wait_recv()

        return carry

    lax.fori_loop(0, nz + 7, loop, 0)

    half = wd_cols // 2

    v_acc[...] = jnp.zeros_like(v_acc)

    def partial(i, carry):
        zz = around(z + nz // 2 + i, nz)
        g = G[zz].reshape(ny * rows, 3 * ff + AUX)
        out = dot(g[:, 0:ff], wg[...], (1, 1)) + dot(g[:, ff:2 * ff], wu[...], (1, 1))
        n = N[zz].reshape(ny * rows, wd_cols).astype(F32)
        aux = g[:, 3 * ff:].astype(F32)
        router = aux[:, 0:1] + aux[:, 1:2]
        v_acc[0] += jnp.sum((out * n).reshape(-1, 8, wd_cols), axis=0)
        v_acc[1] += jnp.sum((n * router).reshape(-1, 8, wd_cols), axis=0)
        out = out.astype(BF)
        t_a[:, zz, :, :, 0:half] = out[:, 0:half].reshape(ny, NC, CAP, half)
        t_a[:, zz, :, :, half:] = g[:, 3 * ff:].reshape(ny, NC, CAP, AUX)
        t_b[zz] = out[:, half:].reshape(ny, NC, CAP, half)
        copy(t_a.at[:, zz, 1 - c], acc_a.at[:, zz], 9, sem_ta.at[zz], partner).start()
        copy(t_b.at[zz, :, 1 - c], acc_b.at[zz], 10, sem_tb.at[zz], partner).start()
        return carry

    lax.fori_loop(0, nz, partial, 0)

    v_own[...] = jnp.sum(v_acc[...], axis=1)
    v_own_copy = copy(v_own, v_core, 15, sem_v.at[0], partner)
    v_own_copy.start()

    def combine(i, carry):
        zz = around(z + nz // 2 + i, nz)
        copy(t_a.at[:, zz, 1 - c], acc_a.at[:, zz], 9, sem_ta.at[zz], partner).wait_recv()
        copy(t_b.at[zz, :, 1 - c], acc_b.at[zz], 10, sem_tb.at[zz], partner).wait_recv()
        acc_a[:, zz] = (acc_a[:, zz].astype(F32) + t_a[:, zz, c].astype(F32)).astype(BF)
        acc_b[zz] = (acc_b[zz].astype(F32) + t_b[zz, :, c].astype(F32)).astype(BF)
        return carry

    lax.fori_loop(0, nz, combine, 0)

    def ring(n, at, get, left, right, sems, send, to):
        top = n // 2

        def add(ref, other):
            ref[...] = (ref[...].astype(F32) + other[...].astype(F32)).astype(BF)

        def start():
            copy(get(around(at + top * way, n)), left.at[top - 1], send, sems.at[0, top - 1], to(way)).start()
            if top > 1:
                copy(get(around(at - (top - 1) * way, n)), right.at[top - 2], send, sems.at[1, top - 2], to(-way)).start()

        def step(r):
            ref = get(around(at + r * way, n))
            copy(ref, left.at[r], send, sems.at[0, r], to(way)).wait_recv()
            add(ref, left.at[r])
            if r > 0:
                copy(ref, left.at[r - 1], send, sems.at[0, r - 1], to(way)).start()
                q = r - 1
                ref = get(around(at - q * way, n))
                copy(ref, right.at[q], send, sems.at[1, q], to(-way)).wait_recv()
                add(ref, right.at[q])
                if q > 0:
                    copy(ref, right.at[q - 1], send, sems.at[1, q - 1], to(-way)).start()

        return start, [functools.partial(step, r) for r in range(top - 1, -1, -1)]

    a1_start, a1 = ring(ny, y, lambda p: acc_a.at[p], a1l, a1s, sem_a1, 11, y_to)
    a2_start, a2 = ring(nz, z, lambda p: acc_a.at[y, p], a2l, a2s, sem_a2, 12, z_to)
    b1_start, b1 = ring(nz, z, lambda p: acc_b.at[p], b1l, b1s, sem_b1, 13, z_to)
    b2_start, b2 = ring(ny, y, lambda p: acc_b.at[z, p], b2l, b2s, sem_b2, 14, y_to)

    def then(first, second):
        def both():
            first()
            second()

        return both

    a_steps = a1[:-1] + [then(a1[-1], a2_start)] + a2
    b_steps = b1[:-1] + [then(b1[-1], b2_start)] + b2

    def v_copy(ref, sem, send, to):
        return copy(ref, ref, send, sem, to)

    def v_first():
        v_own_copy.wait_recv()
        v_y[y] = v_own[...] + v_core[...]
        for d in range(1, ny):
            v_copy(v_y.at[y], sem_vy.at[y], 16, y_to(d)).start()

    def v_second():
        for d in range(1, ny):
            frm = around(y + d, ny)
            v_copy(v_y.at[frm], sem_vy.at[frm], 16, y_to(d)).wait_recv()
        total = v_y[0]
        for k in range(1, ny):
            total = total + v_y[k]
        v_z[z] = total
        for d in range(1, nz):
            v_copy(v_z.at[z], sem_vz.at[z], 17, z_to(d)).start()

    a1_start()
    b1_start()
    counts = U[:, :, :, :, wd_cols:].reshape(-1, AUX).astype(F32)
    count_scale = lax.rsqrt(jnp.sum(counts, axis=0, keepdims=True)[:, 2:3] / CAP)

    tiles = wd_cols // TILE
    schedule = {}
    for k, pick in enumerate(zip(a_steps, b_steps)):
        schedule[k] = list(pick)
    schedule[0].insert(0, v_first)
    schedule[1].insert(0, v_second)
    lag = max(tiles - len(schedule), 0)

    def tile(i, carry):
        columns = pl.ds(pl.multiple_of(i * TILE, TILE), TILE)
        slots = ny * nz * rows
        n = N[:, :, :, :, columns].reshape(slots, TILE)
        u = U[:, :, :, :, columns].reshape(slots, TILE)
        g = G[:, :, :, 0:3 * ff].reshape(slots, 3 * ff)
        both = (dot(n, g[:, 0:2 * ff], (0, 0)) * count_scale).astype(BF)
        grad_gate[columns] = both[:, 0:ff]
        grad_up[columns] = both[:, ff:]
        grad_down[:, columns] = (dot(g[:, 2 * ff:], u, (0, 0)) * count_scale).astype(BF)
        for k, picks in schedule.items():
            @pl.when(i == k + lag)
            def _():
                for pick in picks:
                    pick()
        return carry

    lax.fori_loop(0, max(tiles, len(schedule)), tile, 0)

    for d in range(1, nz):
        frm = around(z + d, nz)
        v_copy(v_z.at[frm], sem_vz.at[frm], 17, z_to(d)).wait_recv()
    sums = v_z[0]
    for k in range(1, nz):
        sums = sums + v_z[k]
    gain_sum, router_sum = sums[0:1], sums[1:2]
    grad_router[...] = count_scale * router_sum
    grad_gain[...] = count_scale * ((gain_sum + rw[...] * router_sum) / gain[...])

    mine = acc_a[y, z].astype(F32)
    router = mine[:, half:half + 1] + mine[:, half + 1:half + 2]
    inner = (mine[:, half + 2:half + 3] + mine[:, half + 3:half + 4]) / width
    d_normed = jnp.concatenate([mine[:, 0:half], acc_b[z, y].astype(F32)], axis=1) + router * rw[...]
    live = lax.broadcasted_iota(jnp.int32, (CAP, AUX), 0) < cnt[...]
    d_picked = inv_o[:, 0:1] * (d_normed * gain[...] - scaled_o[...] * inner)
    d_picked = jnp.where(live[:, 0:1], d_picked, 0.0)
    spread = (lax.broadcasted_iota(jnp.int32, (TOK, CAP), 0) == tok_row[...]).astype(F32).astype(BF)
    high, low = pair(d_picked)
    grad_in[...] = (gro[...].astype(F32) + dot(spread, high, (1, 0)) + dot(spread, low, (1, 0))).astype(BF)

    def drain(ref, send):
        copy(ref, ref, send, sem_sq.at[0], partner).wait_send()

    drain(sq.at[0:3], 0)
    drain(N.at[0, 0:ny - 1, 0], 1)
    drain(N.at[0:nz - 1, :, 0], 2)
    drain(U.at[0:nz - 1, 0, 0], 3)
    drain(U.at[:, 0:ny - 1, 0], 4)
    drain(N.at[:, :, 0], 5)
    drain(U.at[:, :, 0], 6)
    drain(sb.at[:, 0:3], 7)
    drain(G.at[:, 0:3], 8)
    drain(acc_a, 9)
    drain(acc_b, 10)
    drain(acc_a.at[0:ny - 1], 11)
    drain(acc_a.at[0, 0:nz - 1], 12)
    drain(acc_b.at[0:nz - 1], 13)
    drain(acc_b.at[0, 0:ny - 1], 14)
    drain(v_own, 15)
    drain(v_y.at[0:ny - 1], 16)
    drain(v_z.at[0:nz - 1], 17)


def body(hidden_in, grad_out, slot_tokens, live_counts, norm_gain, router_weight, gate_weight, up_weight, down_weight, sizes):
    ny, nz, nx, width = sizes
    cols, ff = gate_weight.shape
    rows = NC * CAP
    half = cols // 2
    vmem = pl.BlockSpec(memory_space=pltpu.VMEM)
    dma = pltpu.SemaphoreType.DMA
    scratch = pltpu.VMEM

    def slots(n):
        return n // 2, max(n // 2 - 1, 1)

    yl, ys = slots(ny)
    zl, zs = slots(nz)
    a, b = half + AUX, half
    tok = jnp.broadcast_to(slot_tokens[:, None], (CAP, TOK))
    tok_row = jnp.broadcast_to(slot_tokens[None], (TOK, CAP))
    cnt = jnp.broadcast_to(live_counts[:, None], (CAP, AUX))
    grad_in, grad_gate, grad_up, grad_down, grad_gain, grad_router = pl.pallas_call(
        functools.partial(kernel, sizes),
        out_shape=(
            jax.ShapeDtypeStruct(grad_out.shape, BF),
            jax.ShapeDtypeStruct((cols, ff), BF),
            jax.ShapeDtypeStruct((cols, ff), BF),
            jax.ShapeDtypeStruct((ff, cols), BF),
            jax.ShapeDtypeStruct((1, cols), F32),
            jax.ShapeDtypeStruct((1, cols), F32),
        ),
        in_specs=[vmem] * 10,
        out_specs=[vmem] * 6,
        scratch_shapes=[
            scratch((nz, ny, NC, CAP, cols), BF),
            scratch((nz, ny, NC, CAP, cols + AUX), BF),
            scratch((nz, nx, rows, 3 * ff + AUX), BF),
            scratch((CAP, cols), F32),
            scratch((CAP, AUX), F32),
            scratch((nx, CAP, AUX), F32),
            scratch((nz, nx, rows, 3 * ff), BF),
            scratch((nz, rows, 3 * ff), BF),
            scratch((nz, rows, 3 * ff), BF),
            scratch((nz, rows, 3 * ff), BF),
            scratch((ny, nz, NC, CAP, a), BF),
            scratch((nz, ny, NC, CAP, b), BF),
            scratch((ny, nz, CAP, a), BF),
            scratch((nz, ny, CAP, b), BF),
            scratch((yl, nz, CAP, a), BF),
            scratch((ys, nz, CAP, a), BF),
            scratch((zl, CAP, a), BF),
            scratch((zs, CAP, a), BF),
            scratch((zl, ny, CAP, b), BF),
            scratch((zs, ny, CAP, b), BF),
            scratch((yl, CAP, b), BF),
            scratch((ys, CAP, b), BF),
            scratch((2, 8, cols), F32),
            scratch((2, cols), F32),
            scratch((2, cols), F32),
            scratch((ny, 2, cols), F32),
            scratch((nz, 2, cols), F32),
            dma((nx,)), dma((nz, ny)), dma((ny,)), dma((nz,)), dma((ny, nz)), dma((nz,)), dma((nz,)),
            dma((nz,)), dma((nz,)), dma((nz,)), dma((nz,)), dma((nz,)), dma((nz,)),
            dma((nz,)), dma((nz,)), dma((2, yl)), dma((2, zl)), dma((2, zl)), dma((2, yl)), dma((1,)), dma((ny,)), dma((nz,)),
            dma((18,)),
        ],
        compiler_params=pltpu.CompilerParams(collective_id=0, has_side_effects=True, vmem_limit_bytes=67000000),
        name="block",
    )(tok, tok_row, cnt, hidden_in, grad_out, norm_gain[None], router_weight[None], gate_weight, up_weight, down_weight)
    return grad_in, grad_gate, grad_up, grad_down, grad_gain[0], grad_router[0]


def solution(mesh):
    nx = mesh.shape["tensor"]
    ny = nx
    nz = mesh.shape["seq"] // (ny * NC)
    weights = (P("tensor", "seq"), P("tensor", "seq"), P("seq", "tensor"))
    in_specs = (P("seq", "tensor"), P("seq", "tensor"), P("seq"), P("seq"), P("tensor"), P("tensor")) + weights
    out_specs = (P("seq", "tensor"),) + weights + (P("tensor"), P("tensor"))

    def whole(hidden_in, *rest):
        sizes = (ny, nz, nx, hidden_in.shape[1] * nx)
        return body(hidden_in, *rest, sizes)

    return jax.shard_map(whole, mesh=mesh, in_specs=in_specs, out_specs=out_specs, check_vma=False)
```

```python
import functools

import jax
import jax.numpy as jnp
from jax import lax
from jax.experimental import pallas as pl
from jax.experimental.pallas import tpu as pltpu
from jax.sharding import PartitionSpec as P

MESH = pl.DeviceIdType.MESH
BF = jnp.bfloat16
F32 = jnp.float32
norm_eps = 1e-06
NC = 2
CAP = 16
AUX = 128
TOK = 128
TILE = 256


def geometry(ny, nz, nx):
    s, t = lax.axis_index("seq"), lax.axis_index("tensor")
    c = lax.rem(s, NC)
    z = lax.rem(s // NC, nz)
    y = s // (NC * nz)
    way = 1 - 2 * c
    return y, z, c, t, way


def around(value, size):
    return lax.rem(value + 8 * size, size)


def step_of(k, way):
    far = (k + 1) // 2
    sign = (2 * lax.rem(k, 2) - 1) * way
    return sign, sign * far


def pair(value):
    high = value.astype(BF)
    return high, (value - high.astype(F32)).astype(BF)


def lanes(rows, columns):
    lane = lax.broadcasted_iota(jnp.int32, (rows, AUX), 1)
    total = jnp.zeros((rows, AUX), F32)
    for k, column in enumerate(columns):
        total = jnp.where(lane == k, jnp.broadcast_to(column, (rows, AUX)), total)
    return total


def dot(a, b, contract):
    return lax.dot_general(a, b, ((contract[0:1], contract[1:2]), ((), ())), preferred_element_type=F32)


def kernel(
    sizes,
    tok_hbm, cnt_hbm, hid_hbm, gro_hbm, gain_hbm, rw_hbm, wg_hbm, wu_hbm, wd_hbm,
    grad_in, grad_gate, grad_up, grad_down, grad_gain, grad_router,
    N, U, G, scaled_at, inv_at,
    sq, sb, rb_a, rb_b, rb_s,
    part, acc, y_far, y_near, z_in, v_acc, v_own, v_core, v_y, v_z,
    sem_sq, sem_nz, sem_ny, sem_uz, sem_uy, sem_dn, sem_du,
    sem_a, sem_b, sem_s, sem_g1, sem_g2, sem_gs,
    sem_t, sem_y, sem_z, sem_v, sem_vy, sem_vz, sent,
    tok, cnt, hid, gro, gain, rw, wg, wu, wd, sem_in,
):
    ny, nz, nx, width = sizes
    y, z, c, t, way = geometry(ny, nz, nx)
    cols = hid.shape[1]
    ff = wg.shape[1]
    rows = NC * CAP
    lag = 9

    def dev(yy, zz, cc, tt):
        return ((yy * nz + zz) * NC + cc, tt)

    def copy(src, dst, send, recv, to):
        return pltpu.make_async_remote_copy(
            src_ref=src, dst_ref=dst, send_sem=sent.at[send], recv_sem=recv, device_id=to, device_id_type=MESH
        )

    def same(ref, send, recv, to):
        return copy(ref, ref, send, recv, to)

    partner = dev(y, z, 1 - c, t)
    y_to = lambda d: dev(around(y + d, ny), z, c, t)
    z_to = lambda d: dev(y, around(z + d, nz), c, t)
    x_to = lambda d: dev(y, z, c, around(t + d, nx))

    loads = [
        pltpu.make_async_copy(far, near, sem_in.at[q])
        for q, (far, near) in enumerate((
            (tok_hbm, tok), (cnt_hbm, cnt), (hid_hbm, hid), (gain_hbm, gain), (rw_hbm, rw), (gro_hbm, gro),
            (wg_hbm, wg), (wu_hbm, wu), (wd_hbm, wd),
        ))
    ]
    for load in loads:
        load.start()
    barrier = pltpu.get_barrier_semaphore()
    peers = [y_to(d) for d in range(1, ny)] + [z_to(d) for d in range(1, nz)] + [x_to(d) for d in range(1, nx)] + [partner]
    for to in peers:
        pl.semaphore_signal(barrier, inc=1, device_id=to, device_id_type=MESH)

    def spread():
        return (lax.broadcasted_iota(jnp.int32, (TOK, CAP), 0) == tok[...]).astype(F32).astype(BF)

    for load in loads[0:5]:
        load.wait()
    live = lax.broadcasted_iota(jnp.int32, (CAP, 1), 0) < cnt[...]
    wide = dot(spread(), hid[...], (0, 0))
    rounded = rw[...].astype(BF).astype(F32)
    s1 = jnp.sum(wide * wide, axis=1, keepdims=True)
    s2 = jnp.sum(wide * (gain[...] * rounded), axis=1, keepdims=True)
    sq[t] = lanes(CAP, (s1, s2))

    pl.semaphore_wait(barrier, len(peers))
    for d in range(1, nx):
        same(sq.at[t], 0, sem_sq.at[t], x_to(d)).start()
    loads[5].wait()
    ups = dot(spread(), gro[...], (0, 0))
    U[z, y, c, :, 0:cols] = jnp.where(live, ups, 0.0).astype(BF)
    v_acc[...] = jnp.zeros_like(v_acc)
    for d in range(1, nx):
        frm = around(t + d, nx)
        same(sq.at[frm], 0, sem_sq.at[frm], x_to(d)).wait_recv()
    total = sq[0]
    for k in range(1, nx):
        total = total + sq[k]
    inverse = lax.rsqrt(total[:, 0:1] / width + norm_eps)
    scaled = wide * inverse
    N[z, y, c] = (scaled * gain[...]).astype(BF)
    scaled_at[...] = scaled
    inv_at[...] = jnp.broadcast_to(inverse, (CAP, AUX))
    high, low = pair(total[:, 1:2] * inverse)
    count = jnp.broadcast_to(cnt[...], (CAP, 1)).astype(F32)
    U[z, y, c, :, cols:] = lanes(CAP, (high.astype(F32), low.astype(F32), count)).astype(BF)

    def n_copy(zz, yy, send, recv, to):
        return same(N.at[zz, yy, c], send, recv, to)

    def u_copy(zz, yy, send, recv, to):
        return same(U.at[zz, yy, c], send, recv, to)

    def n_z_sends(yy):
        n_copy(z, yy, 2, sem_nz.at[1, yy], z_to(way)).start()
        if nz > 2:
            n_copy(z, yy, 2, sem_nz.at[2, yy], z_to(-way)).start()

    def u_y_sends(zz):
        u_copy(zz, y, 4, sem_uy.at[1, zz], y_to(way)).start()
        if ny > 2:
            u_copy(zz, y, 4, sem_uy.at[2, zz], y_to(-way)).start()

    def chunk_z(k):
        return around(z - step_of(k, way)[1], nz)

    def n_y_arrival(m):
        sign, far = step_of(m, way)
        yy = around(y - far, ny)
        n_copy(z, yy, 1, sem_ny.at[m], y_to(sign)).wait_recv()
        if m + 2 < ny:
            n_copy(z, yy, 1, sem_ny.at[m + 2], y_to(sign)).start()
        n_z_sends(yy)

    def u_y_arrival(k, m):
        zz = chunk_z(k)
        sign, far = step_of(m, way)
        yy = around(y - far, ny)
        u_copy(zz, yy, 4, sem_uy.at[m, zz], y_to(sign)).wait_recv()
        if m + 2 < ny:
            u_copy(zz, yy, 4, sem_uy.at[m + 2, zz], y_to(sign)).start()

    n_copy(z, y, 1, sem_ny.at[1], y_to(way)).start()
    if ny > 2:
        n_copy(z, y, 1, sem_ny.at[2], y_to(-way)).start()
    u_copy(z, y, 3, sem_uz.at[1], z_to(way)).start()
    if nz > 2:
        u_copy(z, y, 3, sem_uz.at[2], z_to(-way)).start()
    u_y_sends(z)
    n_z_sends(y)
    for m in range(1, ny):
        n_y_arrival(m)
        u_y_arrival(0, m)
    same(N.at[z, :, c], 5, sem_dn.at[z], partner).start()
    same(U.at[z, :, c], 6, sem_du.at[z], partner).start()

    def within(k, low, high):
        return pl.when((k >= low) & (k < high))

    def upstream_along_z(k):
        @within(k, 1, nz)
        def _():
            sign, far = step_of(k, way)
            zz = around(z - far, nz)
            u_copy(zz, y, 3, sem_uz.at[k], z_to(sign)).wait_recv()

            @pl.when(k + 2 < nz)
            def _():
                u_copy(zz, y, 3, sem_uz.at[k + 2], z_to(sign)).start()

            u_y_sends(zz)

    def upstream_along_y(k):
        @within(k, 1, nz)
        def _():
            for m in range(1, min(ny, 3)):
                u_y_arrival(k, m)

    def upstream_last(k):
        @within(k, 1, nz)
        def _():
            for m in range(3, ny):
                u_y_arrival(k, m)
            zz = chunk_z(k)
            same(U.at[zz, :, c], 6, sem_du.at[zz], partner).start()

    def normed_along_z(k):
        @within(k, 1, nz)
        def _():
            sign, far = step_of(k, way)
            zz = around(z - far, nz)
            for yy in range(ny):
                n_copy(zz, yy, 2, sem_nz.at[k, yy], z_to(sign)).wait_recv()

                @pl.when(k + 2 < nz)
                def _():
                    n_copy(zz, yy, 2, sem_nz.at[k + 2, yy], z_to(sign)).start()

            same(N.at[zz, :, c], 5, sem_dn.at[zz], partner).start()

    def x_block(i, d):
        return sb.at[i, around(t + d, nx)]

    def project(i):
        @within(i, 0, nz)
        def _():
            zz = chunk_z(i)
            same(N.at[zz, :, 1 - c], 5, sem_dn.at[zz], partner).wait_recv()
            same(U.at[zz, :, 1 - c], 6, sem_du.at[zz], partner).wait_recv()
            n = N[zz].reshape(ny * rows, cols)
            u = U[zz, :, :, :, 0:cols].reshape(ny * rows, cols)
            for q, out in enumerate((dot(n, wg[...], (1, 0)), dot(n, wu[...], (1, 0)), dot(u, wd[...], (1, 1)))):
                sb[i, :, :, q * ff:(q + 1) * ff] = out.astype(BF).reshape(nx, rows, ff)
            copy(x_block(i, 2), rb_a.at[i], 7, sem_a.at[i], x_to(way)).start()
            copy(x_block(i, -way), rb_s.at[i], 7, sem_s.at[i], x_to(-way)).start()

    def add(ref, other):
        ref[...] = (ref[...].astype(F32) + other[...].astype(F32)).astype(BF)

    def relay_sum(i):
        @within(i, 0, nz)
        def _():
            block = x_block(i, way)
            copy(block, rb_a.at[i], 7, sem_a.at[i], x_to(way)).wait_recv()
            add(block, rb_a.at[i])
            copy(block, rb_b.at[i], 7, sem_b.at[i], x_to(way)).start()

    def gate_backward(i):
        @within(i, 0, nz)
        def _():
            zz = chunk_z(i)
            block = x_block(i, 0)
            copy(block, rb_b.at[i], 7, sem_b.at[i], x_to(way)).wait_recv()
            copy(block, rb_s.at[i], 7, sem_s.at[i], x_to(-way)).wait_recv()
            full = sb[i, t].astype(F32) + rb_b[i].astype(F32) + rb_s[i].astype(F32)
            gate, upper, back = full[:, 0:ff], full[:, ff:2 * ff], full[:, 2 * ff:]
            aux = U[zz, t, :, :, cols:].reshape(rows, AUX).astype(F32)
            logits = aux[:, 0:1] + aux[:, 1:2]
            sig = jax.nn.sigmoid(gate)
            act = gate * sig
            slope = sig * (1.0 + gate * (1.0 - sig))
            hidden = act * upper
            d_hidden = logits * back
            d_gate = (d_hidden * upper * slope).astype(BF)
            d_up = (d_hidden * act).astype(BF)
            router = jnp.sum(hidden * back, axis=1, keepdims=True)
            inner = jnp.sum(d_gate.astype(F32) * gate + d_up.astype(F32) * upper, axis=1, keepdims=True) + router * logits
            G[zz, t, :, 0:ff] = d_gate
            G[zz, t, :, ff:2 * ff] = d_up
            G[zz, t, :, 2 * ff:3 * ff] = (hidden * logits).astype(BF)
            halves = pair(router) + pair(inner)
            G[zz, t, :, 3 * ff:] = lanes(rows, [v.astype(F32) for v in halves]).astype(BF)
            same(G.at[zz, t], 8, sem_g1.at[i], x_to(way)).start()
            same(G.at[zz, t], 8, sem_gs.at[i], x_to(-way)).start()

    def relay_gradients(i):
        @within(i, 0, nz)
        def _():
            block = G.at[chunk_z(i), around(t - way, nx)]
            same(block, 8, sem_g1.at[i], x_to(way)).wait_recv()
            same(block, 8, sem_g2.at[i], x_to(way)).start()

    def rows_backward(i):
        @within(i, 0, nz)
        def _():
            zz = chunk_z(i)
            same(G.at[zz, around(t + way, nx)], 8, sem_gs.at[i], x_to(-way)).wait_recv()
            same(G.at[zz, around(t + 2, nx)], 8, sem_g2.at[i], x_to(way)).wait_recv()
            g = G[zz].reshape(ny * rows, 3 * ff + AUX)
            out = dot(g[:, 0:ff], wg[...], (1, 1)) + dot(g[:, ff:2 * ff], wu[...], (1, 1))
            part[zz, :, :, :, 0:cols] = out.astype(BF).reshape(ny, NC, CAP, cols)
            part[zz, :, :, :, cols:] = g[:, 3 * ff:].reshape(ny, NC, CAP, AUX)
            copy(part.at[zz, :, 1 - c], acc.at[zz], 9, sem_t.at[zz], partner).start()
            n = N[zz].reshape(ny * rows, cols).astype(F32)
            aux = g[:, 3 * ff:].astype(F32)
            router = aux[:, 0:1] + aux[:, 1:2]
            v_acc[0] += jnp.sum((out * n).reshape(-1, 8, cols), axis=0)
            v_acc[1] += jnp.sum((n * router).reshape(-1, 8, cols), axis=0)

    def y_start(i):
        @within(i, 0, nz)
        def _():
            zz = chunk_z(i)
            copy(part.at[zz, :, 1 - c], acc.at[zz], 9, sem_t.at[zz], partner).wait_recv()
            acc[zz] = (acc[zz].astype(F32) + part[zz, :, c].astype(F32)).astype(BF)
            copy(acc.at[zz, around(y + 2, ny)], y_far.at[zz, 1], 10, sem_y.at[zz, 1], y_to(way)).start()
            copy(acc.at[zz, around(y - way, ny)], y_near.at[zz], 10, sem_y.at[zz, 2], y_to(-way)).start()

    def y_relay(i):
        @within(i, 0, nz)
        def _():
            zz = chunk_z(i)
            block = acc.at[zz, around(y + way, ny)]
            copy(block, y_far.at[zz, 1], 10, sem_y.at[zz, 1], y_to(way)).wait_recv()
            add(block, y_far.at[zz, 1])
            copy(block, y_far.at[zz, 0], 10, sem_y.at[zz, 0], y_to(way)).start()

    def y_end(i):
        @within(i, 0, nz)
        def _():
            zz = chunk_z(i)
            block = acc.at[zz, y]
            copy(block, y_near.at[zz], 10, sem_y.at[zz, 2], y_to(-way)).wait_recv()
            copy(block, y_far.at[zz, 0], 10, sem_y.at[zz, 0], y_to(way)).wait_recv()
            total = block[...].astype(F32) + y_near[zz].astype(F32) + y_far[zz, 0].astype(F32)
            block[...] = total.astype(BF)

            @pl.when(i > 0)
            def _():
                copy(block, z_in.at[z], 11, sem_z.at[z], dev(y, zz, c, t)).start()

            @pl.when(i == 0)
            def _():
                z_in[z] = block[...]

    own_sums = copy(v_own, v_core, 12, sem_v.at[0], partner)

    def sums_start():
        v_own[...] = jnp.sum(v_acc[...], axis=1)
        own_sums.start()

    def sums_y():
        own_sums.wait_recv()
        v_y[y] = v_own[...] + v_core[...]
        for d in range(1, ny):
            same(v_y.at[y], 13, sem_vy.at[y], y_to(d)).start()

    def sums_z():
        for d in range(1, ny):
            frm = around(y + d, ny)
            same(v_y.at[frm], 13, sem_vy.at[frm], y_to(d)).wait_recv()
        total = v_y[0]
        for k in range(1, ny):
            total = total + v_y[k]
        v_z[z] = total
        for d in range(1, nz):
            same(v_z.at[z], 14, sem_vz.at[z], z_to(d)).start()

    def scale():
        counts = U[:, :, :, :, cols:].reshape(-1, AUX).astype(F32)
        return lax.rsqrt(jnp.sum(counts, axis=0, keepdims=True)[:, 2:3] / CAP)

    def tile(i, carry):
        columns = pl.ds(pl.multiple_of(i * TILE, TILE), TILE)
        slots = ny * nz * rows
        n = N[:, :, :, :, columns].reshape(slots, TILE)
        u = U[:, :, :, :, columns].reshape(slots, TILE)
        g = G[:, :, :, 0:3 * ff].reshape(slots, 3 * ff)
        count_scale = scale()
        both = (dot(n, g[:, 0:2 * ff], (0, 0)) * count_scale).astype(BF)
        grad_gate[columns] = both[:, 0:ff]
        grad_up[columns] = both[:, ff:]
        grad_down[:, columns] = (dot(g[:, 2 * ff:], u, (0, 0)) * count_scale).astype(BF)
        return carry

    for load in loads[6:9]:
        load.wait()
    tiles = cols // TILE
    last = nz - 1 + lag
    each = max(tiles // 4, 1)

    def loop(k, carry):
        upstream_along_z(2 * k - 1)
        upstream_along_z(2 * k)
        upstream_along_y(2 * k - 3)
        upstream_along_y(2 * k - 2)
        upstream_last(2 * k - 5)
        upstream_last(2 * k - 4)
        normed_along_z(k)
        rows_backward(k - 6)
        relay_gradients(k - 5)
        gate_backward(k - 4)
        y_end(k - 9)
        y_relay(k - 8)
        y_start(k - 7)
        relay_sum(k - 3)
        project(k - 2)
        pl.when(k == last - 3)(sums_start)
        pl.when(k == last - 2)(sums_y)
        pl.when(k == last - 1)(sums_z)
        begin = jnp.where(k >= last - 3, (k - (last - 3)) * each, 0)
        end = jnp.where(k >= last - 3, begin + each, 0)
        lax.fori_loop(begin, end, tile, 0)
        return carry

    lax.fori_loop(0, last + 1, loop, 0)

    for d in range(1, nz):
        frm = around(z + d, nz)
        same(v_z.at[frm], 14, sem_vz.at[frm], z_to(d)).wait_recv()
    sums = v_z[0]
    for k in range(1, nz):
        sums = sums + v_z[k]
    gain_sum, router_sum = sums[0:1], sums[1:2]
    count_scale = scale()
    grad_router[...] = count_scale * router_sum
    grad_gain[...] = count_scale * ((gain_sum + rw[...] * router_sum) / gain[...])

    for d in range(1, nz):
        frm = around(z + d, nz)
        copy(z_in.at[frm], z_in.at[frm], 11, sem_z.at[frm], z_to(d)).wait_recv()
    mine = z_in[0].astype(F32)
    for k in range(1, nz):
        mine = mine + z_in[k].astype(F32)
    router = mine[:, cols:cols + 1] + mine[:, cols + 1:cols + 2]
    inner = (mine[:, cols + 2:cols + 3] + mine[:, cols + 3:cols + 4]) / width
    d_normed = mine[:, 0:cols] + router * rw[...]
    d_picked = inv_at[:, 0:1] * (d_normed * gain[...] - scaled_at[...] * inner)
    high, low = pair(jnp.where(live, d_picked, 0.0))
    grad_in[...] = (gro[...].astype(F32) + dot(spread(), high, (1, 0)) + dot(spread(), low, (1, 0))).astype(BF)

    def drain(ref, send):
        same(ref, send, sem_sq.at[0], partner).wait_send()

    drain(sq.at[0:nx - 1], 0)
    drain(N.at[0, 0:ny - 1, 0], 1)
    drain(N.at[0:nz - 1, :, 0], 2)
    drain(U.at[0:nz - 1, 0, 0], 3)
    drain(U.at[:, 0:ny - 1, 0], 4)
    drain(N.at[:, :, 0], 5)
    drain(U.at[:, :, 0], 6)
    drain(sb.at[:, 0:3], 7)
    drain(G.at[:, 0:3], 8)
    drain(acc, 9)
    drain(acc.at[:, 0:3], 10)
    drain(z_in.at[0:nz - 1], 11)
    drain(v_own, 12)
    drain(v_y.at[0:ny - 1], 13)
    drain(v_z.at[0:nz - 1], 14)


def body(hidden_in, grad_out, slot_tokens, live_counts, norm_gain, router_weight, gate_weight, up_weight, down_weight, sizes):
    ny, nz, nx, width = sizes
    cols, ff = gate_weight.shape
    rows = NC * CAP
    vmem = pl.BlockSpec(memory_space=pltpu.VMEM)
    dma = pltpu.SemaphoreType.DMA
    scratch = pltpu.VMEM
    grad_in, grad_gate, grad_up, grad_down, grad_gain, grad_router = pl.pallas_call(
        functools.partial(kernel, sizes),
        out_shape=(
            scratch(grad_out.shape, BF),
            scratch((cols, ff), BF),
            scratch((cols, ff), BF),
            scratch((ff, cols), BF),
            scratch((1, cols), F32),
            scratch((1, cols), F32),
        ),
        in_specs=[pl.BlockSpec(memory_space=pltpu.HBM)] * 9,
        out_specs=[vmem] * 6,
        scratch_shapes=[
            scratch((nz, ny, NC, CAP, cols), BF),
            scratch((nz, ny, NC, CAP, cols + AUX), BF),
            scratch((nz, nx, rows, 3 * ff + AUX), BF),
            scratch((CAP, cols), F32),
            scratch((CAP, AUX), F32),
            scratch((nx, CAP, AUX), F32),
            scratch((nz, nx, rows, 3 * ff), BF),
            scratch((nz, rows, 3 * ff), BF),
            scratch((nz, rows, 3 * ff), BF),
            scratch((nz, rows, 3 * ff), BF),
            scratch((nz, ny, NC, CAP, cols + AUX), BF),
            scratch((nz, ny, CAP, cols + AUX), BF),
            scratch((nz, 2, CAP, cols + AUX), BF),
            scratch((nz, CAP, cols + AUX), BF),
            scratch((nz, CAP, cols + AUX), BF),
            scratch((2, 8, cols), F32),
            scratch((2, cols), F32),
            scratch((2, cols), F32),
            scratch((ny, 2, cols), F32),
            scratch((nz, 2, cols), F32),
            dma((nx,)), dma((nz, ny)), dma((ny,)), dma((nz,)), dma((ny, nz)), dma((nz,)), dma((nz,)),
            dma((nz,)), dma((nz,)), dma((nz,)), dma((nz,)), dma((nz,)), dma((nz,)),
            dma((nz,)), dma((nz, 3)), dma((nz,)), dma((1,)), dma((ny,)), dma((nz,)), dma((15,)),
            scratch((1, CAP), jnp.int32), scratch((1, 1), jnp.int32),
            scratch(hidden_in.shape, BF), scratch(grad_out.shape, BF), scratch((1, cols), F32), scratch((1, cols), F32),
            scratch((cols, ff), BF), scratch((cols, ff), BF), scratch((ff, cols), BF), dma((9,)),
        ],
        compiler_params=pltpu.CompilerParams(collective_id=0, has_side_effects=True, vmem_limit_bytes=60000000),
        name="block",
    )(
        slot_tokens[None], live_counts[None], hidden_in, grad_out, norm_gain[None], router_weight[None],
        gate_weight, up_weight, down_weight,
    )
    return grad_in, grad_gate, grad_up, grad_down, grad_gain[0], grad_router[0]


def solution(mesh):
    nx = mesh.shape["tensor"]
    ny = nx
    nz = mesh.shape["seq"] // (ny * NC)
    weights = (P("tensor", "seq"), P("tensor", "seq"), P("seq", "tensor"))
    in_specs = (P("seq", "tensor"), P("seq", "tensor"), P("seq"), P("seq"), P("tensor"), P("tensor")) + weights
    out_specs = (P("seq", "tensor"),) + weights + (P("tensor"), P("tensor"))

    def whole(hidden_in, *rest):
        sizes = (ny, nz, nx, hidden_in.shape[1] * nx)
        return body(hidden_in, *rest, sizes)

    return jax.shard_map(whole, mesh=mesh, in_specs=in_specs, out_specs=out_specs, check_vma=False)
```

```python
import functools

import jax
import jax.numpy as jnp
from jax import lax
from jax.experimental import pallas as pl
from jax.experimental.pallas import tpu as pltpu
from jax.sharding import PartitionSpec as P

MESH = pl.DeviceIdType.MESH
BF = jnp.bfloat16
F32 = jnp.float32
norm_eps = 1e-06
NC = 2
CAP = 16
AUX = 128
TOK = 128
TILE = 256


def geometry(ny, nz, nx):
    s, t = lax.axis_index("seq"), lax.axis_index("tensor")
    c = lax.rem(s, NC)
    z = lax.rem(s // NC, nz)
    y = s // (NC * nz)
    way = 1 - 2 * c
    return y, z, c, t, way


def around(value, size):
    return lax.rem(value + 8 * size, size)


def step_of(k, way):
    far = (k + 1) // 2
    sign = (2 * lax.rem(k, 2) - 1) * way
    return sign, sign * far


def pair(value):
    high = value.astype(BF)
    return high, (value - high.astype(F32)).astype(BF)


def lanes(rows, columns):
    lane = lax.broadcasted_iota(jnp.int32, (rows, AUX), 1)
    total = jnp.zeros((rows, AUX), F32)
    for k, column in enumerate(columns):
        total = jnp.where(lane == k, jnp.broadcast_to(column, (rows, AUX)), total)
    return total


def dot(a, b, contract):
    return lax.dot_general(a, b, ((contract[0:1], contract[1:2]), ((), ())), preferred_element_type=F32)


def kernel(
    sizes,
    tok_hbm, cnt_hbm, hid_hbm, gro_hbm, gain_hbm, rw_hbm, wg_hbm, wu_hbm, wd_hbm,
    grad_in, grad_gate, grad_up, grad_down, grad_gain, grad_router,
    N, NN, U, G, scaled_at, inv_at,
    sq, sb, rb_a, rb_b, rb_s,
    part, acc, y_in, z_in, v_acc, v_own, v_core, v_y, v_z,
    sem_sq, sem_nz, sem_ny, sem_uz, sem_uy, sem_dn, sem_du,
    sem_a, sem_b, sem_s, sem_g1, sem_g2, sem_gs,
    sem_t, sem_y, sem_z, sem_v, sem_vy, sem_vz, sent,
    tok, cnt, hid, gro, gain, rw, wg, wu, wd, sem_in,
):
    ny, nz, nx, width = sizes
    y, z, c, t, way = geometry(ny, nz, nx)
    cols = hid.shape[1]
    ff = wg.shape[1]
    rows = NC * CAP
    lag = 7

    def dev(yy, zz, cc, tt):
        return ((yy * nz + zz) * NC + cc, tt)

    def copy(src, dst, send, recv, to):
        return pltpu.make_async_remote_copy(
            src_ref=src, dst_ref=dst, send_sem=sent.at[send], recv_sem=recv, device_id=to, device_id_type=MESH
        )

    def same(ref, send, recv, to):
        return copy(ref, ref, send, recv, to)

    partner = dev(y, z, 1 - c, t)
    y_to = lambda d: dev(around(y + d, ny), z, c, t)
    z_to = lambda d: dev(y, around(z + d, nz), c, t)
    x_to = lambda d: dev(y, z, c, around(t + d, nx))

    loads = [
        pltpu.make_async_copy(far, near, sem_in.at[q])
        for q, (far, near) in enumerate((
            (tok_hbm, tok), (cnt_hbm, cnt), (hid_hbm, hid), (gain_hbm, gain), (rw_hbm, rw), (gro_hbm, gro),
            (wg_hbm, wg), (wu_hbm, wu), (wd_hbm, wd),
        ))
    ]
    for load in loads:
        load.start()
    barrier = pltpu.get_barrier_semaphore()
    peers = [y_to(d) for d in range(1, ny)] + [z_to(d) for d in range(1, nz)] + [x_to(d) for d in range(1, nx)] + [partner]
    for to in peers:
        pl.semaphore_signal(barrier, inc=1, device_id=to, device_id_type=MESH)

    def spread():
        return (lax.broadcasted_iota(jnp.int32, (TOK, CAP), 0) == tok[...]).astype(F32).astype(BF)

    for load in loads[0:5]:
        load.wait()
    live = lax.broadcasted_iota(jnp.int32, (CAP, 1), 0) < cnt[...]
    wide = dot(spread(), hid[...], (0, 0))
    rounded = rw[...].astype(BF).astype(F32)
    s1 = jnp.sum(wide * wide, axis=1, keepdims=True)
    s2 = jnp.sum(wide * (gain[...] * rounded), axis=1, keepdims=True)
    sq[t] = lanes(CAP, (s1, s2))
    N[z, y, c] = wide.astype(BF)

    def n_copy(zz, yy, send, recv, to):
        return same(N.at[zz, yy, c], send, recv, to)

    def u_copy(zz, yy, send, recv, to):
        return same(U.at[zz, yy, c], send, recv, to)

    def n_z_sends(yy):
        n_copy(z, yy, 2, sem_nz.at[1, yy], z_to(way)).start()
        if nz > 2:
            n_copy(z, yy, 2, sem_nz.at[2, yy], z_to(-way)).start()

    def u_y_sends(zz):
        u_copy(zz, y, 4, sem_uy.at[1, zz], y_to(way)).start()
        if ny > 2:
            u_copy(zz, y, 4, sem_uy.at[2, zz], y_to(-way)).start()

    def chunk_z(k):
        return around(z - step_of(k, way)[1], nz)

    def n_y_arrival(m):
        sign, far = step_of(m, way)
        yy = around(y - far, ny)
        n_copy(z, yy, 1, sem_ny.at[m], y_to(sign)).wait_recv()
        if m + 2 < ny:
            n_copy(z, yy, 1, sem_ny.at[m + 2], y_to(sign)).start()
        n_z_sends(yy)

    def u_y_arrival(k, m):
        zz = chunk_z(k)
        sign, far = step_of(m, way)
        yy = around(y - far, ny)
        u_copy(zz, yy, 4, sem_uy.at[m, zz], y_to(sign)).wait_recv()
        if m + 2 < ny:
            u_copy(zz, yy, 4, sem_uy.at[m + 2, zz], y_to(sign)).start()

    pl.semaphore_wait(barrier, len(peers))
    n_copy(z, y, 1, sem_ny.at[1], y_to(way)).start()
    if ny > 2:
        n_copy(z, y, 1, sem_ny.at[2], y_to(-way)).start()
    for d in range(1, nx):
        same(sq.at[t], 0, sem_sq.at[t], x_to(d)).start()
    n_z_sends(y)
    loads[5].wait()
    ups = dot(spread(), gro[...], (0, 0))
    U[z, y, c, :, 0:cols] = jnp.where(live, ups, 0.0).astype(BF)
    v_acc[...] = jnp.zeros_like(v_acc)
    for d in range(1, nx):
        frm = around(t + d, nx)
        same(sq.at[frm], 0, sem_sq.at[frm], x_to(d)).wait_recv()
    total = sq[0]
    for k in range(1, nx):
        total = total + sq[k]
    inverse = lax.rsqrt(total[:, 0:1] / width + norm_eps)
    scaled_at[...] = wide * inverse
    inv_at[...] = jnp.broadcast_to(inverse, (CAP, AUX))
    count = jnp.broadcast_to(cnt[...], (CAP, 1)).astype(F32)
    halves = [v.astype(F32) for v in pair(total[:, 1:2] * inverse) + pair(inverse)]
    U[z, y, c, :, cols:] = lanes(CAP, halves[0:2] + [count] + halves[2:4]).astype(BF)
    u_y_sends(z)
    u_copy(z, y, 3, sem_uz.at[1], z_to(way)).start()
    if nz > 2:
        u_copy(z, y, 3, sem_uz.at[2], z_to(-way)).start()
    for m in range(1, ny):
        n_y_arrival(m)
    same(N.at[z, :, c], 5, sem_dn.at[z], partner).start()
    for m in range(1, ny):
        u_y_arrival(0, m)
    same(U.at[z, :, c], 6, sem_du.at[z], partner).start()
    for load in loads[6:9]:
        load.wait()

    def within(k, low, high):
        return pl.when((k >= low) & (k < high))

    def upstream_along_z(k):
        @within(k, 1, nz)
        def _():
            sign, far = step_of(k, way)
            zz = around(z - far, nz)
            u_copy(zz, y, 3, sem_uz.at[k], z_to(sign)).wait_recv()

            @pl.when(k + 2 < nz)
            def _():
                u_copy(zz, y, 3, sem_uz.at[k + 2], z_to(sign)).start()

            u_y_sends(zz)

    def upstream_along_y(k):
        @within(k, 1, nz)
        def _():
            for m in range(1, min(ny, 3)):
                u_y_arrival(k, m)

    def upstream_last(k):
        @within(k, 1, nz)
        def _():
            for m in range(3, ny):
                u_y_arrival(k, m)
            zz = chunk_z(k)
            same(U.at[zz, :, c], 6, sem_du.at[zz], partner).start()

    def normed_along_z(k):
        @within(k, 1, nz)
        def _():
            sign, far = step_of(k, way)
            zz = around(z - far, nz)
            for yy in range(ny):
                n_copy(zz, yy, 2, sem_nz.at[k, yy], z_to(sign)).wait_recv()

                @pl.when(k + 2 < nz)
                def _():
                    n_copy(zz, yy, 2, sem_nz.at[k + 2, yy], z_to(sign)).start()

            same(N.at[zz, :, c], 5, sem_dn.at[zz], partner).start()

    def x_block(i, d):
        return sb.at[i, around(t + d, nx)]

    def project(i):
        @within(i, 0, nz)
        def _():
            zz = chunk_z(i)
            same(N.at[zz, :, 1 - c], 5, sem_dn.at[zz], partner).wait_recv()
            same(U.at[zz, :, 1 - c], 6, sem_du.at[zz], partner).wait_recv()
            aux = U[zz, :, :, :, cols:].reshape(ny * rows, AUX).astype(F32)
            inverse = aux[:, 3:4] + aux[:, 4:5]
            n = (N[zz].reshape(ny * rows, cols).astype(F32) * inverse * gain[...]).astype(BF)
            NN[zz] = n.reshape(ny, NC, CAP, cols)
            u = U[zz, :, :, :, 0:cols].reshape(ny * rows, cols)
            for q, out in enumerate((dot(n, wg[...], (1, 0)), dot(n, wu[...], (1, 0)), dot(u, wd[...], (1, 1)))):
                sb[i, :, :, q * ff:(q + 1) * ff] = out.astype(BF).reshape(nx, rows, ff)
            copy(x_block(i, 2), rb_a.at[i], 7, sem_a.at[i], x_to(way)).start()
            copy(x_block(i, -way), rb_s.at[i], 7, sem_s.at[i], x_to(-way)).start()

    def add(ref, other):
        ref[...] = (ref[...].astype(F32) + other[...].astype(F32)).astype(BF)

    def relay_sum(i):
        @within(i, 0, nz)
        def _():
            block = x_block(i, way)
            copy(block, rb_a.at[i], 7, sem_a.at[i], x_to(way)).wait_recv()
            add(block, rb_a.at[i])
            copy(block, rb_b.at[i], 7, sem_b.at[i], x_to(way)).start()

    def gate_backward(i):
        @within(i, 0, nz)
        def _():
            zz = chunk_z(i)
            block = x_block(i, 0)
            copy(block, rb_b.at[i], 7, sem_b.at[i], x_to(way)).wait_recv()
            copy(block, rb_s.at[i], 7, sem_s.at[i], x_to(-way)).wait_recv()
            full = sb[i, t].astype(F32) + rb_b[i].astype(F32) + rb_s[i].astype(F32)
            gate, upper, back = full[:, 0:ff], full[:, ff:2 * ff], full[:, 2 * ff:]
            aux = U[zz, t, :, :, cols:].reshape(rows, AUX).astype(F32)
            logits = aux[:, 0:1] + aux[:, 1:2]
            sig = jax.nn.sigmoid(gate)
            act = gate * sig
            slope = sig * (1.0 + gate * (1.0 - sig))
            hidden = act * upper
            d_hidden = logits * back
            d_gate = (d_hidden * upper * slope).astype(BF)
            d_up = (d_hidden * act).astype(BF)
            router = jnp.sum(hidden * back, axis=1, keepdims=True)
            inner = jnp.sum(d_gate.astype(F32) * gate + d_up.astype(F32) * upper, axis=1, keepdims=True) + router * logits
            G[zz, t, :, 0:ff] = d_gate
            G[zz, t, :, ff:2 * ff] = d_up
            G[zz, t, :, 2 * ff:3 * ff] = (hidden * logits).astype(BF)
            halves = pair(router) + pair(inner)
            G[zz, t, :, 3 * ff:] = lanes(rows, [v.astype(F32) for v in halves]).astype(BF)
            same(G.at[zz, t], 8, sem_g1.at[i], x_to(way)).start()
            same(G.at[zz, t], 8, sem_gs.at[i], x_to(-way)).start()

    def relay_gradients(i):
        @within(i, 0, nz)
        def _():
            block = G.at[chunk_z(i), around(t - way, nx)]
            same(block, 8, sem_g1.at[i], x_to(way)).wait_recv()
            same(block, 8, sem_g2.at[i], x_to(way)).start()

    def rows_backward(i):
        @within(i, 0, nz)
        def _():
            zz = chunk_z(i)
            same(G.at[zz, around(t + way, nx)], 8, sem_gs.at[i], x_to(-way)).wait_recv()
            same(G.at[zz, around(t + 2, nx)], 8, sem_g2.at[i], x_to(way)).wait_recv()
            g = G[zz].reshape(ny * rows, 3 * ff + AUX)
            out = dot(g[:, 0:ff], wg[...], (1, 1)) + dot(g[:, ff:2 * ff], wu[...], (1, 1))
            part[zz, :, :, :, 0:cols] = out.astype(BF).reshape(ny, NC, CAP, cols)
            part[zz, :, :, :, cols:] = g[:, 3 * ff:].reshape(ny, NC, CAP, AUX)
            copy(part.at[zz, :, 1 - c], acc.at[zz], 9, sem_t.at[zz], partner).start()
            n = NN[zz].reshape(ny * rows, cols).astype(F32)
            aux = g[:, 3 * ff:].astype(F32)
            router = aux[:, 0:1] + aux[:, 1:2]
            v_acc[0] += jnp.sum((out * n).reshape(-1, 8, cols), axis=0)
            v_acc[1] += jnp.sum((n * router).reshape(-1, 8, cols), axis=0)

    def y_start(i):
        @within(i, 0, nz)
        def _():
            zz = chunk_z(i)
            copy(part.at[zz, :, 1 - c], acc.at[zz], 9, sem_t.at[zz], partner).wait_recv()
            acc[zz] = (acc[zz].astype(F32) + part[zz, :, c].astype(F32)).astype(BF)
            for d in range(1, ny):
                yy = around(y + d, ny)
                copy(acc.at[zz, yy], y_in.at[zz, d - 1], 10, sem_y.at[zz, d - 1], y_to(d)).start()

    def y_end(i):
        @within(i, 0, nz)
        def _():
            zz = chunk_z(i)
            block = acc.at[zz, y]
            for d in range(1, ny):
                copy(block, y_in.at[zz, d - 1], 10, sem_y.at[zz, d - 1], y_to(d)).wait_recv()
            total = block[...].astype(F32)
            for d in range(1, ny):
                total = total + y_in[zz, d - 1].astype(F32)
            block[...] = total.astype(BF)

            @pl.when(i > 0)
            def _():
                copy(block, z_in.at[z], 11, sem_z.at[z], dev(y, zz, c, t)).start()

            @pl.when(i == 0)
            def _():
                z_in[z] = block[...]

    own_sums = copy(v_own, v_core, 12, sem_v.at[0], partner)

    def sums_start():
        v_own[...] = jnp.sum(v_acc[...], axis=1)
        own_sums.start()

    def sums_y():
        own_sums.wait_recv()
        v_y[y] = v_own[...] + v_core[...]
        for d in range(1, ny):
            same(v_y.at[y], 13, sem_vy.at[y], y_to(d)).start()

    def sums_z():
        for d in range(1, ny):
            frm = around(y + d, ny)
            same(v_y.at[frm], 13, sem_vy.at[frm], y_to(d)).wait_recv()
        total = v_y[0]
        for k in range(1, ny):
            total = total + v_y[k]
        v_z[z] = total
        for d in range(1, nz):
            same(v_z.at[z], 14, sem_vz.at[z], z_to(d)).start()

    def scale():
        counts = U[:, :, :, :, cols:].reshape(-1, AUX).astype(F32)
        return lax.rsqrt(jnp.sum(counts, axis=0, keepdims=True)[:, 2:3] / CAP)

    def tile(i, carry):
        columns = pl.ds(pl.multiple_of(i * TILE, TILE), TILE)
        slots = ny * nz * rows
        n = NN[:, :, :, :, columns].reshape(slots, TILE)
        u = U[:, :, :, :, columns].reshape(slots, TILE)
        g = G[:, :, :, 0:3 * ff].reshape(slots, 3 * ff)
        count_scale = scale()
        both = (dot(n, g[:, 0:2 * ff], (0, 0)) * count_scale).astype(BF)
        grad_gate[columns] = both[:, 0:ff]
        grad_up[columns] = both[:, ff:]
        grad_down[:, columns] = (dot(g[:, 2 * ff:], u, (0, 0)) * count_scale).astype(BF)
        return carry

    tiles = cols // TILE
    last = nz - 1 + lag
    each = -(-tiles // 3)

    def early(k, late):
        return jnp.where(k == late - 1, 0, jnp.where(k == late, -1, k - late))

    def loop(k, carry):
        upstream_along_z(2 * k + 1)
        upstream_along_z(2 * k + 2)
        upstream_along_y(2 * k - 1)
        upstream_along_y(2 * k)
        upstream_last(2 * k - 3)
        upstream_last(2 * k - 2)
        normed_along_z(k + 1)
        project(early(k, 1))
        relay_sum(early(k, 2))
        gate_backward(early(k, 3))
        relay_gradients(early(k, 4))
        rows_backward(early(k, 5))
        y_start(early(k, 6))
        y_end(early(k, 7))
        pl.when(k == last - 2)(sums_start)
        pl.when(k == last - 1)(sums_y)
        pl.when(k == last)(sums_z)
        begin = jnp.clip((k - (last - 2)) * each, 0, tiles)
        end = jnp.clip((k - (last - 3)) * each, 0, tiles)
        lax.fori_loop(begin, end, tile, 0)
        return carry

    lax.fori_loop(0, last + 1, loop, 0)

    for d in range(1, nz):
        frm = around(z + d, nz)
        same(v_z.at[frm], 14, sem_vz.at[frm], z_to(d)).wait_recv()
    sums = v_z[0]
    for k in range(1, nz):
        sums = sums + v_z[k]
    gain_sum, router_sum = sums[0:1], sums[1:2]
    count_scale = scale()
    grad_router[...] = count_scale * router_sum
    grad_gain[...] = count_scale * ((gain_sum + rw[...] * router_sum) / gain[...])

    for d in range(1, nz):
        frm = around(z + d, nz)
        copy(z_in.at[frm], z_in.at[frm], 11, sem_z.at[frm], z_to(d)).wait_recv()
    mine = z_in[0].astype(F32)
    for k in range(1, nz):
        mine = mine + z_in[k].astype(F32)
    router = mine[:, cols:cols + 1] + mine[:, cols + 1:cols + 2]
    inner = (mine[:, cols + 2:cols + 3] + mine[:, cols + 3:cols + 4]) / width
    d_normed = mine[:, 0:cols] + router * rw[...]
    d_picked = inv_at[:, 0:1] * (d_normed * gain[...] - scaled_at[...] * inner)
    high, low = pair(jnp.where(live, d_picked, 0.0))
    grad_in[...] = (gro[...].astype(F32) + dot(spread(), high, (1, 0)) + dot(spread(), low, (1, 0))).astype(BF)

    def drain(ref, send):
        same(ref, send, sem_sq.at[0], partner).wait_send()

    drain(sq.at[0:nx - 1], 0)
    drain(N.at[0, 0:ny - 1, 0], 1)
    drain(N.at[0:nz - 1, :, 0], 2)
    drain(U.at[0:nz - 1, 0, 0], 3)
    drain(U.at[:, 0:ny - 1, 0], 4)
    drain(N.at[:, :, 0], 5)
    drain(U.at[:, :, 0], 6)
    drain(sb.at[:, 0:3], 7)
    drain(G.at[:, 0:3], 8)
    drain(acc, 9)
    drain(acc.at[:, 0:ny - 1], 10)
    drain(z_in.at[0:nz - 1], 11)
    drain(v_own, 12)
    drain(v_y.at[0:ny - 1], 13)
    drain(v_z.at[0:nz - 1], 14)


def body(hidden_in, grad_out, slot_tokens, live_counts, norm_gain, router_weight, gate_weight, up_weight, down_weight, sizes):
    ny, nz, nx, width = sizes
    cols, ff = gate_weight.shape
    rows = NC * CAP
    vmem = pl.BlockSpec(memory_space=pltpu.VMEM)
    dma = pltpu.SemaphoreType.DMA
    scratch = pltpu.VMEM
    grad_in, grad_gate, grad_up, grad_down, grad_gain, grad_router = pl.pallas_call(
        functools.partial(kernel, sizes),
        out_shape=(
            scratch(grad_out.shape, BF),
            scratch((cols, ff), BF),
            scratch((cols, ff), BF),
            scratch((ff, cols), BF),
            scratch((1, cols), F32),
            scratch((1, cols), F32),
        ),
        in_specs=[pl.BlockSpec(memory_space=pltpu.HBM)] * 9,
        out_specs=[vmem] * 6,
        scratch_shapes=[
            scratch((nz, ny, NC, CAP, cols), BF),
            scratch((nz, ny, NC, CAP, cols), BF),
            scratch((nz, ny, NC, CAP, cols + AUX), BF),
            scratch((nz, nx, rows, 3 * ff + AUX), BF),
            scratch((CAP, cols), F32),
            scratch((CAP, AUX), F32),
            scratch((nx, CAP, AUX), F32),
            scratch((nz, nx, rows, 3 * ff), BF),
            scratch((nz, rows, 3 * ff), BF),
            scratch((nz, rows, 3 * ff), BF),
            scratch((nz, rows, 3 * ff), BF),
            scratch((nz, ny, NC, CAP, cols + AUX), BF),
            scratch((nz, ny, CAP, cols + AUX), BF),
            scratch((nz, ny - 1, CAP, cols + AUX), BF),
            scratch((nz, CAP, cols + AUX), BF),
            scratch((2, 8, cols), F32),
            scratch((2, cols), F32),
            scratch((2, cols), F32),
            scratch((ny, 2, cols), F32),
            scratch((nz, 2, cols), F32),
            dma((nx,)), dma((nz, ny)), dma((ny,)), dma((nz,)), dma((ny, nz)), dma((nz,)), dma((nz,)),
            dma((nz,)), dma((nz,)), dma((nz,)), dma((nz,)), dma((nz,)), dma((nz,)),
            dma((nz,)), dma((nz, ny - 1)), dma((nz,)), dma((1,)), dma((ny,)), dma((nz,)), dma((15,)),
            scratch((1, CAP), jnp.int32), scratch((1, 1), jnp.int32),
            scratch(hidden_in.shape, BF), scratch(grad_out.shape, BF), scratch((1, cols), F32), scratch((1, cols), F32),
            scratch((cols, ff), BF), scratch((cols, ff), BF), scratch((ff, cols), BF), dma((9,)),
        ],
        compiler_params=pltpu.CompilerParams(collective_id=0, has_side_effects=True, vmem_limit_bytes=60000000),
        name="block",
    )(
        slot_tokens[None], live_counts[None], hidden_in, grad_out, norm_gain[None], router_weight[None],
        gate_weight, up_weight, down_weight,
    )
    return grad_in, grad_gate, grad_up, grad_down, grad_gain[0], grad_router[0]


def solution(mesh):
    nx = mesh.shape["tensor"]
    ny = nx
    nz = mesh.shape["seq"] // (ny * NC)
    weights = (P("tensor", "seq"), P("tensor", "seq"), P("seq", "tensor"))
    in_specs = (P("seq", "tensor"), P("seq", "tensor"), P("seq"), P("seq"), P("tensor"), P("tensor")) + weights
    out_specs = (P("seq", "tensor"),) + weights + (P("tensor"), P("tensor"))

    def whole(hidden_in, *rest):
        sizes = (ny, nz, nx, hidden_in.shape[1] * nx)
        return body(hidden_in, *rest, sizes)

    return jax.shard_map(whole, mesh=mesh, in_specs=in_specs, out_specs=out_specs, check_vma=False)
```

```python
import functools

import jax
import jax.numpy as jnp
from jax import lax
from jax.experimental import pallas as pl
from jax.experimental.pallas import tpu as pltpu
from jax.sharding import PartitionSpec as P

MESH = pl.DeviceIdType.MESH
BF = jnp.bfloat16
F32 = jnp.float32
norm_eps = 1e-06
NC = 2
CAP = 16
AUX = 128
TOK = 128
TILE = 256


def geometry(ny, nz, nx):
    s, t = lax.axis_index("seq"), lax.axis_index("tensor")
    c = lax.rem(s, NC)
    z = lax.rem(s // NC, nz)
    y = s // (NC * nz)
    way = 1 - 2 * c
    return y, z, c, t, way


def around(value, size):
    return lax.rem(value + 8 * size, size)


def step_of(k, way):
    far = (k + 1) // 2
    sign = (2 * lax.rem(k, 2) - 1) * way
    return sign, sign * far


def pair(value):
    high = value.astype(BF)
    return high, (value - high.astype(F32)).astype(BF)


def lanes(rows, columns):
    lane = lax.broadcasted_iota(jnp.int32, (rows, AUX), 1)
    total = jnp.zeros((rows, AUX), F32)
    for k, column in enumerate(columns):
        total = jnp.where(lane == k, jnp.broadcast_to(column, (rows, AUX)), total)
    return total


def dot(a, b, contract):
    return lax.dot_general(a, b, ((contract[0:1], contract[1:2]), ((), ())), preferred_element_type=F32)


def kernel(
    sizes,
    tok_hbm, cnt_hbm, hid_hbm, gro_hbm, gain_hbm, rw_hbm, wg_hbm, wu_hbm, wd_hbm,
    grad_in, grad_gate, grad_up, grad_down, grad_gain, grad_router,
    N, NN, U, G, scaled_at, inv_at,
    sq, sb, rb_a, rb_b, rb_s,
    part, acc, y_in, z_in, v_acc, v_own, v_core, v_y, v_z,
    sem_sq, sem_nz, sem_ny, sem_uz, sem_uy, sem_dn, sem_du,
    sem_a, sem_b, sem_s, sem_g1, sem_g2, sem_gs,
    sem_t, sem_y, sem_z, sem_v, sem_vy, sem_vz, sent,
    tok, cnt, hid, gro, gain, rw, wg, wu, wd, wg_t, wu_t, sem_in,
):
    ny, nz, nx, width = sizes
    y, z, c, t, way = geometry(ny, nz, nx)
    cols = hid.shape[1]
    ff = wg.shape[1]
    rows = NC * CAP
    lag = 7

    def dev(yy, zz, cc, tt):
        return ((yy * nz + zz) * NC + cc, tt)

    def copy(src, dst, send, recv, to):
        return pltpu.make_async_remote_copy(
            src_ref=src, dst_ref=dst, send_sem=sent.at[send], recv_sem=recv, device_id=to, device_id_type=MESH
        )

    def same(ref, send, recv, to):
        return copy(ref, ref, send, recv, to)

    partner = dev(y, z, 1 - c, t)
    y_to = lambda d: dev(around(y + d, ny), z, c, t)
    z_to = lambda d: dev(y, around(z + d, nz), c, t)
    x_to = lambda d: dev(y, z, c, around(t + d, nx))

    loads = [
        pltpu.make_async_copy(far, near, sem_in.at[q])
        for q, (far, near) in enumerate((
            (tok_hbm, tok), (cnt_hbm, cnt), (hid_hbm, hid), (gain_hbm, gain), (rw_hbm, rw), (gro_hbm, gro),
            (wg_hbm, wg), (wu_hbm, wu), (wd_hbm, wd),
        ))
    ]
    for load in loads:
        load.start()
    barrier = pltpu.get_barrier_semaphore()
    peers = [y_to(d) for d in range(1, ny)] + [z_to(d) for d in range(1, nz)] + [x_to(d) for d in range(1, nx)] + [partner]
    for to in peers:
        pl.semaphore_signal(barrier, inc=1, device_id=to, device_id_type=MESH)

    def spread():
        return (lax.broadcasted_iota(jnp.int32, (TOK, CAP), 0) == tok[...]).astype(F32).astype(BF)

    for load in loads[0:5]:
        load.wait()
    live = lax.broadcasted_iota(jnp.int32, (CAP, 1), 0) < cnt[...]
    wide = dot(spread(), hid[...], (0, 0))
    rounded = rw[...].astype(BF).astype(F32)
    s1 = jnp.sum(wide * wide, axis=1, keepdims=True)
    s2 = jnp.sum(wide * (gain[...] * rounded), axis=1, keepdims=True)
    sq[t] = lanes(CAP, (s1, s2))
    N[z, y, c] = wide.astype(BF)

    def n_copy(zz, yy, send, recv, to):
        return same(N.at[zz, yy, c], send, recv, to)

    def u_copy(zz, yy, send, recv, to):
        return same(U.at[zz, yy, c], send, recv, to)

    def n_z_sends(yy):
        n_copy(z, yy, 2, sem_nz.at[1, yy], z_to(way)).start()
        if nz > 2:
            n_copy(z, yy, 2, sem_nz.at[2, yy], z_to(-way)).start()

    def u_y_sends(zz):
        u_copy(zz, y, 4, sem_uy.at[1, zz], y_to(way)).start()
        if ny > 2:
            u_copy(zz, y, 4, sem_uy.at[2, zz], y_to(-way)).start()

    def chunk_z(k):
        return around(z - step_of(k, way)[1], nz)

    def n_y_arrival(m):
        sign, far = step_of(m, way)
        yy = around(y - far, ny)
        n_copy(z, yy, 1, sem_ny.at[m], y_to(sign)).wait_recv()
        if m + 2 < ny:
            n_copy(z, yy, 1, sem_ny.at[m + 2], y_to(sign)).start()
        n_z_sends(yy)

    def u_y_arrival(k, m):
        zz = chunk_z(k)
        sign, far = step_of(m, way)
        yy = around(y - far, ny)
        u_copy(zz, yy, 4, sem_uy.at[m, zz], y_to(sign)).wait_recv()
        if m + 2 < ny:
            u_copy(zz, yy, 4, sem_uy.at[m + 2, zz], y_to(sign)).start()

    pl.semaphore_wait(barrier, len(peers))
    n_copy(z, y, 1, sem_ny.at[1], y_to(way)).start()
    if ny > 2:
        n_copy(z, y, 1, sem_ny.at[2], y_to(-way)).start()
    for d in range(1, nx):
        same(sq.at[t], 0, sem_sq.at[t], x_to(d)).start()
    n_z_sends(y)
    loads[5].wait()
    ups = dot(spread(), gro[...], (0, 0))
    U[z, y, c, :, 0:cols] = jnp.where(live, ups, 0.0).astype(BF)
    v_acc[...] = jnp.zeros_like(v_acc)
    for d in range(1, nx):
        frm = around(t + d, nx)
        same(sq.at[frm], 0, sem_sq.at[frm], x_to(d)).wait_recv()
    total = sq[0]
    for k in range(1, nx):
        total = total + sq[k]
    inverse = lax.rsqrt(total[:, 0:1] / width + norm_eps)
    scaled_at[...] = wide * inverse
    inv_at[...] = jnp.broadcast_to(inverse, (CAP, AUX))
    count = jnp.broadcast_to(cnt[...], (CAP, 1)).astype(F32)
    halves = [v.astype(F32) for v in pair(total[:, 1:2] * inverse) + pair(inverse)]
    U[z, y, c, :, cols:] = lanes(CAP, halves[0:2] + [count] + halves[2:4]).astype(BF)
    u_y_sends(z)
    u_copy(z, y, 3, sem_uz.at[1], z_to(way)).start()
    if nz > 2:
        u_copy(z, y, 3, sem_uz.at[2], z_to(-way)).start()
    for m in range(1, ny):
        n_y_arrival(m)
    same(N.at[z, :, c], 5, sem_dn.at[z], partner).start()
    for m in range(1, ny):
        u_y_arrival(0, m)
    same(U.at[z, :, c], 6, sem_du.at[z], partner).start()
    for load in loads[6:9]:
        load.wait()

    def within(k, low, high):
        return pl.when((k >= low) & (k < high))

    def upstream_along_z(k):
        @within(k, 1, nz)
        def _():
            sign, far = step_of(k, way)
            zz = around(z - far, nz)
            u_copy(zz, y, 3, sem_uz.at[k], z_to(sign)).wait_recv()

            @pl.when(k + 2 < nz)
            def _():
                u_copy(zz, y, 3, sem_uz.at[k + 2], z_to(sign)).start()

            u_y_sends(zz)

    def upstream_along_y(k):
        @within(k, 1, nz)
        def _():
            for m in range(1, min(ny, 3)):
                u_y_arrival(k, m)

    def upstream_last(k):
        @within(k, 1, nz)
        def _():
            for m in range(3, ny):
                u_y_arrival(k, m)
            zz = chunk_z(k)
            same(U.at[zz, :, c], 6, sem_du.at[zz], partner).start()

    def normed_along_z(k):
        @within(k, 1, nz)
        def _():
            sign, far = step_of(k, way)
            zz = around(z - far, nz)
            for yy in range(ny):
                n_copy(zz, yy, 2, sem_nz.at[k, yy], z_to(sign)).wait_recv()

                @pl.when(k + 2 < nz)
                def _():
                    n_copy(zz, yy, 2, sem_nz.at[k + 2, yy], z_to(sign)).start()

            same(N.at[zz, :, c], 5, sem_dn.at[zz], partner).start()

    def x_block(i, d):
        return sb.at[i, around(t + d, nx)]

    def project(i):
        @within(i, 0, nz)
        def _():
            zz = chunk_z(i)
            same(N.at[zz, :, 1 - c], 5, sem_dn.at[zz], partner).wait_recv()
            same(U.at[zz, :, 1 - c], 6, sem_du.at[zz], partner).wait_recv()
            aux = U[zz, :, :, :, cols:].reshape(ny * rows, AUX).astype(F32)
            inverse = aux[:, 3:4] + aux[:, 4:5]
            n = (N[zz].reshape(ny * rows, cols).astype(F32) * inverse * gain[...]).astype(BF)
            NN[zz] = n.reshape(ny, NC, CAP, cols)
            u = U[zz, :, :, :, 0:cols].reshape(ny * rows, cols)
            for q, out in enumerate((dot(n, wg[...], (1, 0)), dot(n, wu[...], (1, 0)), dot(u, wd[...], (1, 1)))):
                sb[i, :, :, q * ff:(q + 1) * ff] = out.astype(BF).reshape(nx, rows, ff)
            copy(x_block(i, 2), rb_a.at[i], 7, sem_a.at[i], x_to(way)).start()
            copy(x_block(i, -way), rb_s.at[i], 7, sem_s.at[i], x_to(-way)).start()

    def add(ref, other):
        ref[...] = (ref[...].astype(F32) + other[...].astype(F32)).astype(BF)

    def relay_sum(i):
        @within(i, 0, nz)
        def _():
            block = x_block(i, way)
            copy(block, rb_a.at[i], 7, sem_a.at[i], x_to(way)).wait_recv()
            add(block, rb_a.at[i])
            copy(block, rb_b.at[i], 7, sem_b.at[i], x_to(way)).start()

    def gate_backward(i):
        @within(i, 0, nz)
        def _():
            zz = chunk_z(i)
            block = x_block(i, 0)
            copy(block, rb_b.at[i], 7, sem_b.at[i], x_to(way)).wait_recv()
            copy(block, rb_s.at[i], 7, sem_s.at[i], x_to(-way)).wait_recv()
            full = sb[i, t].astype(F32) + rb_b[i].astype(F32) + rb_s[i].astype(F32)
            gate, upper, back = full[:, 0:ff], full[:, ff:2 * ff], full[:, 2 * ff:]
            aux = U[zz, t, :, :, cols:].reshape(rows, AUX).astype(F32)
            logits = aux[:, 0:1] + aux[:, 1:2]
            sig = jax.nn.sigmoid(gate)
            act = gate * sig
            slope = sig * (1.0 + gate * (1.0 - sig))
            hidden = act * upper
            d_hidden = logits * back
            d_gate = (d_hidden * upper * slope).astype(BF)
            d_up = (d_hidden * act).astype(BF)
            router = jnp.sum(hidden * back, axis=1, keepdims=True)
            inner = jnp.sum(d_gate.astype(F32) * gate + d_up.astype(F32) * upper, axis=1, keepdims=True) + router * logits
            G[zz, t, :, 0:ff] = d_gate
            G[zz, t, :, ff:2 * ff] = d_up
            G[zz, t, :, 2 * ff:3 * ff] = (hidden * logits).astype(BF)
            halves = pair(router) + pair(inner)
            G[zz, t, :, 3 * ff:] = lanes(rows, [v.astype(F32) for v in halves]).astype(BF)
            same(G.at[zz, t], 8, sem_g1.at[i], x_to(way)).start()
            same(G.at[zz, t], 8, sem_gs.at[i], x_to(-way)).start()

    def relay_gradients(i):
        @within(i, 0, nz)
        def _():
            block = G.at[chunk_z(i), around(t - way, nx)]
            same(block, 8, sem_g1.at[i], x_to(way)).wait_recv()
            same(block, 8, sem_g2.at[i], x_to(way)).start()

    def rows_backward(i):
        @within(i, 0, nz)
        def _():
            zz = chunk_z(i)
            same(G.at[zz, around(t + way, nx)], 8, sem_gs.at[i], x_to(-way)).wait_recv()
            same(G.at[zz, around(t + 2, nx)], 8, sem_g2.at[i], x_to(way)).wait_recv()
            g = G[zz].reshape(ny * rows, 3 * ff + AUX)
            out = dot(g[:, 0:ff], wg_t[...], (1, 0)) + dot(g[:, ff:2 * ff], wu_t[...], (1, 0))
            part[zz, :, :, :, 0:cols] = out.astype(BF).reshape(ny, NC, CAP, cols)
            part[zz, :, :, :, cols:] = g[:, 3 * ff:].reshape(ny, NC, CAP, AUX)
            copy(part.at[zz, :, 1 - c], acc.at[zz], 9, sem_t.at[zz], partner).start()
            n = NN[zz].reshape(ny * rows, cols).astype(F32)
            aux = g[:, 3 * ff:].astype(F32)
            router = aux[:, 0:1] + aux[:, 1:2]
            v_acc[0] += jnp.sum((out * n).reshape(-1, 8, cols), axis=0)
            v_acc[1] += jnp.sum((n * router).reshape(-1, 8, cols), axis=0)

    def y_start(i):
        @within(i, 0, nz)
        def _():
            zz = chunk_z(i)
            copy(part.at[zz, :, 1 - c], acc.at[zz], 9, sem_t.at[zz], partner).wait_recv()
            acc[zz] = (acc[zz].astype(F32) + part[zz, :, c].astype(F32)).astype(BF)
            for d in range(1, ny):
                yy = around(y + d, ny)
                copy(acc.at[zz, yy], y_in.at[zz, d - 1], 10, sem_y.at[zz, d - 1], y_to(d)).start()

    def y_end(i):
        @within(i, 0, nz)
        def _():
            zz = chunk_z(i)
            block = acc.at[zz, y]
            for d in range(1, ny):
                copy(block, y_in.at[zz, d - 1], 10, sem_y.at[zz, d - 1], y_to(d)).wait_recv()
            total = block[...].astype(F32)
            for d in range(1, ny):
                total = total + y_in[zz, d - 1].astype(F32)
            block[...] = total.astype(BF)

            @pl.when(i > 0)
            def _():
                copy(block, z_in.at[z], 11, sem_z.at[z], dev(y, zz, c, t)).start()

            @pl.when(i == 0)
            def _():
                z_in[z] = block[...]

    own_sums = copy(v_own, v_core, 12, sem_v.at[0], partner)

    def sums_start():
        v_own[...] = jnp.sum(v_acc[...], axis=1)
        own_sums.start()

    def sums_y():
        own_sums.wait_recv()
        v_y[y] = v_own[...] + v_core[...]
        for d in range(1, ny):
            same(v_y.at[y], 13, sem_vy.at[y], y_to(d)).start()

    def sums_z():
        for d in range(1, ny):
            frm = around(y + d, ny)
            same(v_y.at[frm], 13, sem_vy.at[frm], y_to(d)).wait_recv()
        total = v_y[0]
        for k in range(1, ny):
            total = total + v_y[k]
        v_z[z] = total
        for d in range(1, nz):
            same(v_z.at[z], 14, sem_vz.at[z], z_to(d)).start()

    def scale():
        counts = U[:, :, :, :, cols:].reshape(-1, AUX).astype(F32)
        return lax.rsqrt(jnp.sum(counts, axis=0, keepdims=True)[:, 2:3] / CAP)

    def tile(i, carry):
        columns = pl.ds(pl.multiple_of(i * TILE, TILE), TILE)
        slots = ny * nz * rows
        n = NN[:, :, :, :, columns].reshape(slots, TILE)
        u = U[:, :, :, :, columns].reshape(slots, TILE)
        g = G[:, :, :, 0:3 * ff].reshape(slots, 3 * ff)
        count_scale = scale()
        both = (dot(n, g[:, 0:2 * ff], (0, 0)) * count_scale).astype(BF)
        grad_gate[columns] = both[:, 0:ff]
        grad_up[columns] = both[:, ff:]
        grad_down[:, columns] = (dot(g[:, 2 * ff:], u, (0, 0)) * count_scale).astype(BF)
        return carry

    def flip_gate():
        wg_t[...] = wg[...].T

    def flip_up():
        wu_t[...] = wu[...].T

    tiles = cols // TILE
    last = nz - 1 + lag
    each = -(-tiles // 3)

    def early(k, late):
        return jnp.where(k == late - 1, 0, jnp.where(k == late, -1, k - late))

    def loop(k, carry):
        upstream_along_z(2 * k + 1)
        upstream_along_z(2 * k + 2)
        upstream_along_y(2 * k - 1)
        upstream_along_y(2 * k)
        upstream_last(2 * k - 3)
        upstream_last(2 * k - 2)
        normed_along_z(k + 1)
        project(early(k, 1))
        relay_sum(early(k, 2))
        gate_backward(early(k, 3))
        relay_gradients(early(k, 4))
        rows_backward(early(k, 5))
        y_start(early(k, 6))
        y_end(early(k, 7))
        pl.when(k == 1)(flip_gate)
        pl.when(k == 2)(flip_up)
        pl.when(k == last - 2)(sums_start)
        pl.when(k == last - 1)(sums_y)
        pl.when(k == last)(sums_z)
        begin = jnp.clip((k - (last - 2)) * 2, 0, tiles)
        end = jnp.where(k == last, tiles, jnp.clip((k - (last - 3)) * 2, 0, tiles))
        lax.fori_loop(begin, end, tile, 0)
        return carry

    lax.fori_loop(0, last + 1, loop, 0)

    for d in range(1, nz):
        frm = around(z + d, nz)
        same(v_z.at[frm], 14, sem_vz.at[frm], z_to(d)).wait_recv()
    sums = v_z[0]
    for k in range(1, nz):
        sums = sums + v_z[k]
    gain_sum, router_sum = sums[0:1], sums[1:2]
    count_scale = scale()
    grad_router[...] = count_scale * router_sum
    grad_gain[...] = count_scale * ((gain_sum + rw[...] * router_sum) / gain[...])

    for d in range(1, nz):
        frm = around(z + d, nz)
        copy(z_in.at[frm], z_in.at[frm], 11, sem_z.at[frm], z_to(d)).wait_recv()
    mine = z_in[0].astype(F32)
    for k in range(1, nz):
        mine = mine + z_in[k].astype(F32)
    router = mine[:, cols:cols + 1] + mine[:, cols + 1:cols + 2]
    inner = (mine[:, cols + 2:cols + 3] + mine[:, cols + 3:cols + 4]) / width
    d_normed = mine[:, 0:cols] + router * rw[...]
    d_picked = inv_at[:, 0:1] * (d_normed * gain[...] - scaled_at[...] * inner)
    high, low = pair(jnp.where(live, d_picked, 0.0))
    grad_in[...] = (gro[...].astype(F32) + dot(spread(), high, (1, 0)) + dot(spread(), low, (1, 0))).astype(BF)

    def drain(ref, send):
        same(ref, send, sem_sq.at[0], partner).wait_send()

    drain(sq.at[0:nx - 1], 0)
    drain(N.at[0, 0:ny - 1, 0], 1)
    drain(N.at[0:nz - 1, :, 0], 2)
    drain(U.at[0:nz - 1, 0, 0], 3)
    drain(U.at[:, 0:ny - 1, 0], 4)
    drain(N.at[:, :, 0], 5)
    drain(U.at[:, :, 0], 6)
    drain(sb.at[:, 0:3], 7)
    drain(G.at[:, 0:3], 8)
    drain(acc, 9)
    drain(acc.at[:, 0:ny - 1], 10)
    drain(z_in.at[0:nz - 1], 11)
    drain(v_own, 12)
    drain(v_y.at[0:ny - 1], 13)
    drain(v_z.at[0:nz - 1], 14)


def body(hidden_in, grad_out, slot_tokens, live_counts, norm_gain, router_weight, gate_weight, up_weight, down_weight, sizes):
    ny, nz, nx, width = sizes
    cols, ff = gate_weight.shape
    rows = NC * CAP
    vmem = pl.BlockSpec(memory_space=pltpu.VMEM)
    dma = pltpu.SemaphoreType.DMA
    scratch = pltpu.VMEM
    grad_in, grad_gate, grad_up, grad_down, grad_gain, grad_router = pl.pallas_call(
        functools.partial(kernel, sizes),
        out_shape=(
            scratch(grad_out.shape, BF),
            scratch((cols, ff), BF),
            scratch((cols, ff), BF),
            scratch((ff, cols), BF),
            scratch((1, cols), F32),
            scratch((1, cols), F32),
        ),
        in_specs=[pl.BlockSpec(memory_space=pltpu.HBM)] * 9,
        out_specs=[vmem] * 6,
        scratch_shapes=[
            scratch((nz, ny, NC, CAP, cols), BF),
            scratch((nz, ny, NC, CAP, cols), BF),
            scratch((nz, ny, NC, CAP, cols + AUX), BF),
            scratch((nz, nx, rows, 3 * ff + AUX), BF),
            scratch((CAP, cols), F32),
            scratch((CAP, AUX), F32),
            scratch((nx, CAP, AUX), F32),
            scratch((nz, nx, rows, 3 * ff), BF),
            scratch((nz, rows, 3 * ff), BF),
            scratch((nz, rows, 3 * ff), BF),
            scratch((nz, rows, 3 * ff), BF),
            scratch((nz, ny, NC, CAP, cols + AUX), BF),
            scratch((nz, ny, CAP, cols + AUX), BF),
            scratch((nz, ny - 1, CAP, cols + AUX), BF),
            scratch((nz, CAP, cols + AUX), BF),
            scratch((2, 8, cols), F32),
            scratch((2, cols), F32),
            scratch((2, cols), F32),
            scratch((ny, 2, cols), F32),
            scratch((nz, 2, cols), F32),
            dma((nx,)), dma((nz, ny)), dma((ny,)), dma((nz,)), dma((ny, nz)), dma((nz,)), dma((nz,)),
            dma((nz,)), dma((nz,)), dma((nz,)), dma((nz,)), dma((nz,)), dma((nz,)),
            dma((nz,)), dma((nz, ny - 1)), dma((nz,)), dma((1,)), dma((ny,)), dma((nz,)), dma((15,)),
            scratch((1, CAP), jnp.int32), scratch((1, 1), jnp.int32),
            scratch(hidden_in.shape, BF), scratch(grad_out.shape, BF), scratch((1, cols), F32), scratch((1, cols), F32),
            scratch((cols, ff), BF), scratch((cols, ff), BF), scratch((ff, cols), BF),
            scratch((ff, cols), BF), scratch((ff, cols), BF), dma((9,)),
        ],
        compiler_params=pltpu.CompilerParams(collective_id=0, has_side_effects=True, vmem_limit_bytes=60000000),
        name="block",
    )(
        slot_tokens[None], live_counts[None], hidden_in, grad_out, norm_gain[None], router_weight[None],
        gate_weight, up_weight, down_weight,
    )
    return grad_in, grad_gate, grad_up, grad_down, grad_gain[0], grad_router[0]


def solution(mesh):
    nx = mesh.shape["tensor"]
    ny = nx
    nz = mesh.shape["seq"] // (ny * NC)
    weights = (P("tensor", "seq"), P("tensor", "seq"), P("seq", "tensor"))
    in_specs = (P("seq", "tensor"), P("seq", "tensor"), P("seq"), P("seq"), P("tensor"), P("tensor")) + weights
    out_specs = (P("seq", "tensor"),) + weights + (P("tensor"), P("tensor"))

    def whole(hidden_in, *rest):
        sizes = (ny, nz, nx, hidden_in.shape[1] * nx)
        return body(hidden_in, *rest, sizes)

    return jax.shard_map(whole, mesh=mesh, in_specs=in_specs, out_specs=out_specs, check_vma=False)
```
